256 devices in a mesh: groups: 2 (over z), cells: 128 (over y, x, core).
Axes of the slice: x: 8, y: 8, z: 2, core: 2. Of those that a mesh axis runs over, the one named last changes fastest.
The devices are a block of a 8x8x16 slice.
Arguments:
- pair_act: bfloat16 [768, 384, 128], P(('groups', 'cells')), parts along dimension 0, may hold values from -6 to 6
- pair_mask: int32 [768, 384], P(('groups', 'cells')), parts along dimension 0, may hold values from 0 to 1, as said below
- chain_ids: int32 [768], P('groups'), parts along dimension 0, may hold values from 0 to 3, never falling along the last dimension, each value on 1 to 192 neighbouring positions
- proj_weight: bfloat16 [128, 256], replicated, may hold values from -0.5 to 0.5
- gate_weight: bfloat16 [128, 128], replicated, may hold values from -0.5 to 0.5
- chain_bias: float32 [2, 128], replicated, may hold values from -4 to 4
- out_weight: bfloat16 [64, 128], replicated, may hold values from -0.75 to 0.75
- out_grad: bfloat16 [768, 384, 128], P(('groups', 'cells')), parts along dimension 0, may hold values from -6 to 6
Outputs:
- pair_grad: bfloat16 [768, 384, 128], P(('groups', 'cells')), parts along dimension 0
- proj_weight_grad: float32 [256, 256], P('groups'), parts along dimension 0
- gate_weight_grad: float32 [256, 128], P('groups'), parts along dimension 0
- out_weight_grad: float32 [128, 128], P('groups'), parts along dimension 0
The draws below stay inside these ranges and needn't reach their ends.
There are 2 independent parts, one for each index of `groups`. The reference program is written for one: setup_inputs(seed, part) draws one part's arguments, and reference() takes and returns one part's arrays. A program takes and returns all parts, laid end to end along the dimension named above; an argument that names none is the same for every part. Nothing has to cross between parts.
Inputs may be any that keep to these rules, and one draw needn't show every extreme that they name: pair_mask[i, j] = valid[i] * valid[j] for a 0 or 1 validity of each residue.
All inputs are finite; a program needn't handle non-finite values.
Results may differ from the reference program's by a relative error of at most 0.012.
Values may be sent and summed in bfloat16 or wider, within the bound.
A program may use at most 64 MiB of HBM per device.

```python
import math
import jax
import jax.numpy as jnp
import numpy as np
from jax import lax

C = 128
H = 64
N = 384
N_CELLS = 128


def draw_pair_mask(key, part):
    valid = (jax.random.randint(jax.random.fold_in(key, 11), (N,), 0, 8) < 7).astype(jnp.int32)
    return valid[:, None] * valid[None, :]


def level_of(own_key, extent, pieces, low, top_value):
    gain, own = 1.0, jax.random.fold_in(own_key, 6)
    for dim, blocks in pieces:
        steps = jnp.exp(jax.random.uniform(jax.random.fold_in(own, dim), (blocks,), jnp.float32, low / len(pieces), top_value / len(pieces)))
        gain = gain * jnp.repeat(steps, extent[dim] // blocks).reshape([-1 if axis == dim else 1 for axis in range(len(extent))])
    return gain


def length_profile(number_of, total, bound, slope):
    weights = [(1 << 20) // math.isqrt(rank ** slope) + 1 for rank in range(2, number_of + 1)]
    rest, given = total - bound - (number_of - 1), [1] * (number_of - 1)
    while rest > 0:
        movable = [i for i in range(number_of - 1) if given[i] < bound]
        whole, budget = sum([weights[i] for i in movable]), rest
        for i in movable:
            addition = min(bound - given[i], max(1, budget * weights[i] // whole), rest)
            given[i] = given[i] + addition
            rest = rest - addition
    return np.array([bound] + given)


def uneven(own_key, number_of, total, bound, skew):
    if number_of == 2:
        one = jax.random.randint(own_key, (), max(1, total - bound), min(bound, total - 1) + 1)
        return jnp.stack([one, total - one])
    sizes = jnp.asarray(length_profile(number_of, total, bound, skew), jnp.int32)
    twos = (number_of - 1) // 2
    donor, sink = sizes[1:1 + 2 * twos:2], sizes[2:2 + 2 * twos:2]
    slack = jnp.minimum(donor - 1, bound - sink)
    shifted = jax.random.randint(jax.random.fold_in(own_key, 1), (twos,), 0, 1 << 20) % (slack + 1)
    sizes = sizes.at[1:1 + 2 * twos:2].set(donor - shifted).at[2:2 + 2 * twos:2].set(sink + shifted)
    return sizes[jax.random.permutation(jax.random.fold_in(own_key, 2), number_of)]


def noise(stream_key, shape, spread, limit, cuts=(), kind=jnp.bfloat16):
    gain = level_of(stream_key, shape, cuts, -0.22, 0.18) if cuts else 1.0
    result = jax.random.normal(stream_key, shape, jnp.float32) * spread * gain
    return jnp.minimum(jnp.maximum(result, -limit), limit).astype(kind)


def setup_inputs(seed: int = 0, part: int = 0) -> dict:
    keys = jax.random.split(jax.random.key(seed), 9)
    part_keys = jax.random.split(jax.random.fold_in(keys[8], part), 9)
    pair_act = noise(part_keys[0], (N, N, C), 1.0, 6.0, ((0, 128),))
    pair_mask = draw_pair_mask(jax.random.fold_in(jax.random.fold_in(keys[8], part), 71), part)
    chain_ids = jnp.searchsorted(jnp.cumsum(uneven(part_keys[2], 4, N, N // 2, 0)), jnp.arange(N), side="right").astype(jnp.int32)
    proj_weight = noise(keys[3], (C, 4 * H), C ** -0.5, 0.5)
    gate_weight = noise(keys[4], (C, C), C ** -0.5, 0.5)
    chain_bias = noise(keys[5], (2, C), 1.0, 4.0, (), jnp.float32)
    out_weight = noise(keys[6], (H, C), H ** -0.5, 0.75)
    out_grad = noise(part_keys[7], (N, N, C), 1.0, 6.0, ((0, 128),))
    return {"pair_act": pair_act, "pair_mask": pair_mask, "chain_ids": chain_ids, "proj_weight": proj_weight, "gate_weight": gate_weight, "chain_bias": chain_bias, "out_weight": out_weight, "out_grad": out_grad}


EPS = 1e-05

def matmul(left, right):
    return jnp.dot(left.astype(jnp.float32), right.astype(jnp.float32), precision=lax.Precision.HIGHEST)

def normalize_last(values):
    center = values - lax.optimization_barrier(jnp.mean(values, axis=-1, keepdims=True))
    scale = lax.rsqrt(lax.optimization_barrier(jnp.mean(center * center, axis=-1, keepdims=True)) + EPS)
    return (center * scale, scale)

def norm_backward(grad, normed, scale):
    first = lax.optimization_barrier(jnp.mean(grad, axis=-1, keepdims=True))
    second = lax.optimization_barrier(jnp.mean(grad * normed, axis=-1, keepdims=True))
    return scale * (grad - first - normed * second)

def reference(pair_act, pair_mask, chain_ids, proj_weight, gate_weight, chain_bias, out_weight, out_grad):
    rows = N // N_CELLS
    count = rows * N
    starts = jnp.arange(N_CELLS, dtype=jnp.int32) * rows

    def front(start):
        block = lax.dynamic_slice_in_dim(pair_act, start, rows, 0).astype(jnp.float32).reshape(count, C)
        normed, scale = normalize_last(block)
        normed_low = normed.astype(jnp.bfloat16)
        projected = matmul(normed_low, proj_weight)
        keeper = lax.dynamic_slice_in_dim(pair_mask, start, rows, 0).astype(jnp.float32).reshape(count, 1)
        values = projected[:, :2 * H]
        sigma = jax.nn.sigmoid(projected[:, 2 * H:])
        return (normed, scale, normed_low, values, sigma, keeper)

    def make_factors(start):
        parts = front(start)
        return (parts[5] * parts[4] * parts[3]).astype(jnp.bfloat16)
    stacked = lax.map(make_factors, starts)
    channel_major = jnp.transpose(stacked.reshape(N, N, 2 * H), (2, 0, 1))

    def product(index):
        left_rows = channel_major[index]
        right_rows = channel_major[index + H]
        return matmul(left_rows, right_rows.T)
    triangle = lax.map(product, jnp.arange(H, dtype=jnp.int32))

    def middle(carry, start):
        normed, scale, normed_low, values, sigma, keeper = front(start)
        block = lax.dynamic_slice_in_dim(triangle, start, rows, 1).reshape(H, count).T
        tri_hat, tri_scale = normalize_last(block)
        tri_low = tri_hat.astype(jnp.bfloat16)
        outputs = matmul(tri_low, out_weight)
        own_chain = lax.dynamic_slice_in_dim(chain_ids, start, rows, 0)
        same_chain = (own_chain[:, None] == chain_ids[None, :]).reshape(count, 1)
        logits = matmul(normed_low, gate_weight)
        logits = logits + jnp.where(same_chain, chain_bias[0][None, :], chain_bias[1][None, :])
        gating = jax.nn.sigmoid(logits)
        upstream = lax.dynamic_slice_in_dim(out_grad, start, rows, 0).astype(jnp.float32).reshape(count, C)
        d_outputs = (upstream * gating).astype(jnp.bfloat16)
        d_logits = (upstream * outputs * gating * (1.0 - gating)).astype(jnp.bfloat16)
        out_acc = carry[0] + matmul(tri_low.T, d_outputs)
        gate_acc = carry[1] + matmul(normed_low.T, d_logits)
        d_hat = matmul(d_outputs, out_weight.T)
        d_tri = norm_backward(d_hat, tri_hat, tri_scale).astype(jnp.bfloat16)
        return ((out_acc, gate_acc), (d_tri.T.reshape(H, rows, N), d_logits))
    initial = (jnp.zeros((H, C), jnp.float32), jnp.zeros((C, C), jnp.float32))
    (out_acc, gate_acc), (tri_blocks, logit_blocks) = lax.scan(middle, initial, starts)
    tri_grad = jnp.transpose(tri_blocks, (1, 0, 2, 3)).reshape(H, N, N)

    def back_product(index):
        cotangent = tri_grad[index]
        left_rows = channel_major[index]
        right_rows = channel_major[index + H]
        d_left = matmul(cotangent, right_rows)
        d_right = matmul(cotangent.T, left_rows)
        return (d_left.astype(jnp.bfloat16), d_right.astype(jnp.bfloat16))
    left_grads, right_grads = lax.map(back_product, jnp.arange(H, dtype=jnp.int32))
    factor_grad = jnp.concatenate([left_grads, right_grads], axis=0)

    def finish(carry, inputs):
        start, d_logits = inputs
        normed, scale, normed_low, values, sigma, keeper = front(start)
        d_factor = lax.dynamic_slice_in_dim(factor_grad, start, rows, 1).reshape(2 * H, count).T.astype(jnp.float32)
        d_values = d_factor * keeper * sigma
        d_gates = d_factor * keeper * values * sigma * (1.0 - sigma)
        d_proj = jnp.concatenate([d_values, d_gates], axis=1).astype(jnp.bfloat16)
        proj_acc = carry + matmul(normed_low.T, d_proj)
        d_normed = matmul(d_proj, proj_weight.T)
        d_normed = d_normed + matmul(d_logits, gate_weight.T)
        d_block = norm_backward(d_normed, normed, scale)
        return (proj_acc, d_block.astype(jnp.bfloat16).reshape(rows, N, C))
    proj_acc, grad_blocks = lax.scan(finish, jnp.zeros((C, 4 * H), jnp.float32), (starts, logit_blocks))
    pair_grad = grad_blocks.reshape(N, N, C)
    factor = 1.0 / N
    return (pair_grad, proj_acc * factor, gate_acc * factor, out_acc * factor)
```

```python
import jax
import jax.numpy as jnp
from jax import lax
from jax.experimental import pallas as pl
from jax.experimental.pallas import tpu as pltpu
from jax.sharding import PartitionSpec as P

EPS = 1e-05
MESH = pl.DeviceIdType.MESH
F32 = jnp.float32
BF16 = jnp.bfloat16
LANES = 128
NT = (((1,), (1,)), ((), ()))
TN = (((0,), (0,)), ((), ()))
NN = (((1,), (0,)), ((), ()))


def dot(a, b, dims):
    return lax.dot_general(a, b, dims, preferred_element_type=F32)


def loop(n, body, unroll=1):
    def step(i, carry):
        body(i)
        return carry

    lax.fori_loop(0, n, step, 0, unroll=unroll)


def kernel(
    act_ref,
    grad_ref,
    mask_ref,
    chain_ref,
    own_ref,
    proj_ref,
    gate_ref,
    bias_ref,
    outw_ref,
    pair_out,
    proj_out,
    gate_out,
    out_out,
    zhat_s,
    zscale_s,
    norm_s,
    p1_s,
    p2_s,
    do_s,
    e_s,
    dh_s,
    dl_s,
    dn_s,
    trilow_s,
    dproj_s,
    spread,
    wide,
    flat,
    a_s,
    b_s,
    dt_s,
    s1,
    r1,
    r1p,
    s2,
    r2,
    s3,
    r3,
    s4,
    r4,
    half_s,
    half_r,
    w_s,
    wp_r,
    ws,
    wr,
    gs,
    gr,
    wfin,
    wfin_r,
    send_sem,
    recv_sem,
    pair_send,
    pair_recv,
):
    me = lax.axis_index("cells")
    devices = lax.axis_size("cells")
    chips = devices // 2
    chip = me // 2
    core = lax.rem(me, 2)
    partner = me + 1 - 2 * core
    rows, length = mask_ref.shape[0], mask_ref.shape[2]
    width = act_ref.shape[1]
    hidden = outw_ref.shape[0]
    parts = length // LANES
    chunks = rows * parts
    tall = hidden // 8
    groups = chips // 8

    barrier = pltpu.get_barrier_semaphore()

    def greet(p):
        peer = lax.rem(chip + p + 1, chips) * 2 + core
        pl.semaphore_signal(barrier, inc=1, device_id={"cells": peer}, device_id_type=MESH)

    loop(chips - 1, greet)
    pl.semaphore_signal(barrier, inc=1, device_id={"cells": partner}, device_id_type=MESH)

    def exchange(src, dst, k):
        def one(p):
            t = lax.rem(chip + p + 1, chips)
            pltpu.make_async_remote_copy(
                src_ref=src.at[t],
                dst_ref=dst.at[chip],
                send_sem=send_sem.at[k],
                recv_sem=recv_sem.at[k],
                device_id={"cells": t * 2 + core},
                device_id_type=MESH,
            ).start()

        loop(chips - 1, one)
        pltpu.make_async_copy(src.at[chip], dst.at[chip], recv_sem.at[k]).start()

    def arrive(dst, k):
        pltpu.make_async_copy(dst, dst, recv_sem.at[k]).wait()

    def sent(src, k):
        view = src.at[pl.ds(0, chips - 1)]
        pltpu.make_async_copy(view, view, send_sem.at[k]).wait()

    def to_partner(src, dst, k):
        copy = pltpu.make_async_remote_copy(
            src_ref=src,
            dst_ref=dst,
            send_sem=pair_send.at[k],
            recv_sem=pair_recv.at[k],
            device_id={"cells": partner},
            device_id_type=MESH,
        )
        copy.start()
        return copy

    def cols(q):
        return pl.ds(pl.multiple_of(q * LANES, LANES), LANES)

    def unpack(src, dst):
        n = src.shape[1]

        def one(t):
            at = pl.ds(pl.multiple_of(t * 8, 8), n)
            for kq in range(parts):
                dst[kq, at, :] = src[t, :, kq * LANES : (kq + 1) * LANES].astype(F32)

        loop(chips, one, unroll=4)

    def pack(src, dst):
        n = dst.shape[1]

        def one(t):
            at = pl.ds(pl.multiple_of(t * 8, 8), n)
            for kq in range(parts):
                dst[t, :, kq * LANES : (kq + 1) * LANES] = src[kq, at, :].astype(BF16)

        loop(chips, one, unroll=4)

    def pack_rows(src, dst, at):
        def one(t):
            for kq in range(parts):
                dst[t, at : at + 4, kq * LANES : (kq + 1) * LANES] = src[
                    kq, pl.ds(t, 4, stride=chips), :
                ].astype(BF16)

        loop(chips, one, unroll=4)

    def gather_rows(src, offset, dst):
        for r in range(rows):
            for g in range(0, groups, 2):
                for kq in range(parts):
                    both = [
                        src[kq, pl.ds((g + e) * 64 + offset + r, 8, stride=8), :] for e in range(2)
                    ]
                    dst[
                        r * chips + g * 8 : r * chips + g * 8 + 16, kq * LANES : (kq + 1) * LANES
                    ] = jnp.concatenate(both, axis=0).astype(BF16)

    eye = (
        lax.broadcasted_iota(jnp.int32, (width, width), 0)
        == lax.broadcasted_iota(jnp.int32, (width, width), 1)
    ).astype(BF16)

    def front(q):
        r = q // parts
        kq = lax.rem(q, parts)
        z = dot(eye, act_ref[cols(q), :], NT)
        center = z - jnp.mean(z, axis=0, keepdims=True)
        scale = lax.rsqrt(jnp.mean(center * center, axis=0, keepdims=True) + EPS)
        zhat = center * scale
        low = zhat.astype(BF16)
        zhat_s[:, cols(q)] = zhat
        zscale_s[:, cols(q)] = scale
        norm_s[:, cols(q)] = low
        projected = dot(proj_ref[...], low, TN)
        keeper = mask_ref[r, :, cols(kq)].astype(F32)
        values = projected[: 2 * hidden]
        sigma = jax.nn.sigmoid(projected[2 * hidden :])
        p1 = keeper * sigma
        factors = p1 * values
        p1_s[:, cols(q)] = p1
        p2_s[:, cols(q)] = factors * (1.0 - sigma)
        for ab in range(2):
            for g in range(tall):
                at = ab * hidden + g * 8
                spread[kq, pl.ds(g * 64 + ab * 4 + r, 8, stride=8), :] = factors[at : at + 8]

    loop(chunks, front)
    pack(spread, s1)
    pl.semaphore_wait(barrier, chips)
    exchange(s1, r1, 0)

    def gating(q):
        r = q // parts
        kq = lax.rem(q, parts)
        same = chain_ref[:, cols(kq)] == own_ref[me * rows + r]
        logits = dot(gate_ref[...], norm_s[:, cols(q)], TN)
        logits = logits + jnp.where(same, bias_ref[:, 0:1], bias_ref[:, 1:2])
        gate = jax.nn.sigmoid(logits)
        up = dot(eye, grad_ref[cols(q), :], NT) * gate
        low = up.astype(BF16)
        do_s[:, cols(q)] = low
        e_s[:, cols(q)] = up * (1.0 - gate)
        dh_s[:, cols(q)] = dot(outw_ref[...], low, NN)

    loop(chunks, gating)

    arrive(r1, 0)
    first = to_partner(r1, r1p, 0)
    unpack(r1, spread)
    gather_rows(spread, 0, a_s)

    def place_right(src, which):
        for r in range(rows):
            for g in range(groups):
                for kq in range(parts):
                    wide[kq, pl.ds(g * 48 + 3 * which + r, 8, stride=6), :] = src[
                        kq, pl.ds(g * 64 + 4 + r, 8, stride=8), :
                    ]

    place_right(spread, core)
    first.wait()
    unpack(r1p, spread)
    place_right(spread, 1 - core)
    for kq in range(parts):
        b_s[:, kq * LANES : (kq + 1) * LANES] = wide[kq].astype(BF16)
    for kq in range(parts):
        flat[kq, : rows * chips, :] = dot(
            a_s[...], b_s[kq * LANES : (kq + 1) * LANES, :], NT
        )
    pack_rows(flat, s2, 0)
    exchange(s2, r2, 1)

    arrive(r2, 1)
    unpack(r2, spread)

    def middle(q):
        r = q // parts
        kq = lax.rem(q, parts)
        tri = jnp.concatenate(
            [spread[kq, pl.ds(g * 64 + r, 8, stride=8), :] for g in range(tall)], axis=0
        )
        center = tri - jnp.mean(tri, axis=0, keepdims=True)
        scale = lax.rsqrt(jnp.mean(center * center, axis=0, keepdims=True) + EPS)
        hat = center * scale
        low = hat.astype(BF16)
        trilow_s[:, cols(q)] = low
        outputs = dot(outw_ref[...], low, TN)
        dl_s[:, cols(q)] = (outputs * e_s[:, cols(q)]).astype(BF16)
        d_hat = dh_s[:, cols(q)]
        m1 = jnp.mean(d_hat, axis=0, keepdims=True)
        m2 = jnp.mean(d_hat * hat, axis=0, keepdims=True)
        d_tri = scale * (d_hat - m1 - hat * m2)
        for g in range(tall):
            spread[kq, pl.ds(g * 64 + 4 + r, 8, stride=8), :] = d_tri[g * 8 : g * 8 + 8]

    loop(chunks, middle)

    def pack_upper(t):
        at = pl.ds(pl.multiple_of(t * 8, 8), 8)
        for kq in range(parts):
            s3[t, :, kq * LANES : (kq + 1) * LANES] = spread[kq, at, :][4:8].astype(BF16)

    loop(chips, pack_upper, unroll=4)
    exchange(s3, r3, 2)

    w_s[0:width, :] = dot(norm_s[...], dl_s[...], NT)
    w_s[width : width + hidden, :] = dot(trilow_s[...], do_s[...], NT)
    w_s[width + hidden : 2 * width, :] = jnp.zeros((width - hidden, width), F32)

    def gate_part(q):
        dn_s[:, cols(q)] = dot(gate_ref[...], dl_s[:, cols(q)], NN)

    loop(chunks, gate_part)

    arrive(r3, 2)
    unpack(r3, spread)
    gather_rows(spread, 0, dt_s)
    for kq in range(parts):
        wide[kq] = dot(dt_s[...], a_s[:, kq * LANES : (kq + 1) * LANES], TN)
    for r in range(rows):
        for g in range(groups):
            for kq in range(parts):
                half_s[kq, r * chips + g * 8 : r * chips + g * 8 + 8, :] = wide[
                    kq, pl.ds(g * 48 + 3 * (1 - core) + r, 8, stride=6), :
                ]
    second = to_partner(half_s, half_r, 1)
    for kq in range(parts):
        flat[kq, : rows * chips, :] = dot(
            dt_s[...], b_s[:, kq * LANES : (kq + 1) * LANES], NN
        )
    pack_rows(flat, s4, 0)
    second.wait()
    for r in range(rows):
        for g in range(groups):
            for kq in range(parts):
                at = slice(r * chips + g * 8, r * chips + g * 8 + 8)
                flat[kq, at, :] = (
                    wide[kq, pl.ds(g * 48 + 3 * core + r, 8, stride=6), :] + half_r[kq, at, :]
                )
    pack_rows(flat, s4, 4)
    exchange(s4, r4, 3)

    arrive(r4, 3)
    unpack(r4, spread)

    def factor_back(q):
        r = q // parts
        kq = lax.rem(q, parts)
        d_factors = jnp.concatenate(
            [
                spread[kq, pl.ds(g * 64 + ab * 4 + r, 8, stride=8), :]
                for ab in range(2)
                for g in range(tall)
            ],
            axis=0,
        )
        dproj_s[: 2 * hidden, cols(q)] = (d_factors * p1_s[:, cols(q)]).astype(BF16)
        dproj_s[2 * hidden :, cols(q)] = (d_factors * p2_s[:, cols(q)]).astype(BF16)

    loop(chunks, factor_back)
    for e in range(2):
        w_s[2 * width + e * width : 3 * width + e * width, :] = dot(
            norm_s[...], dproj_s[e * width : (e + 1) * width, :], NT
        )

    quarter = 4 * chips
    here = pl.ds(pl.multiple_of(core * quarter, 8), quarter)
    there = pl.ds(pl.multiple_of((1 - core) * quarter, 8), quarter)
    third = to_partner(w_s.at[there], wp_r, 2)

    def finish(q):
        d_norm = dot(proj_ref[...], dproj_s[:, cols(q)], NN) + dn_s[:, cols(q)]
        zhat = zhat_s[:, cols(q)]
        m1 = jnp.mean(d_norm, axis=0, keepdims=True)
        m2 = jnp.mean(d_norm * zhat, axis=0, keepdims=True)
        grad = zscale_s[:, cols(q)] * (d_norm - m1 - zhat * m2)
        pair_out[cols(q), :] = grad.T.astype(BF16)

    third.wait()
    wp_r[...] = w_s[here, :] + wp_r[...]

    def split(t):
        ws[t] = wp_r[pl.ds(t, 4, stride=chips), :]

    loop(chips, split, unroll=4)
    exchange(ws, wr, 4)
    loop(chunks, finish)
    arrive(wr, 4)
    total = jnp.sum(wr[...], axis=0) * (1.0 / length)
    gs[...] = total

    def spread_total(p):
        t = lax.rem(chip + p + 1, chips)
        pltpu.make_async_remote_copy(
            src_ref=gs,
            dst_ref=gr.at[chip],
            send_sem=send_sem.at[5],
            recv_sem=recv_sem.at[5],
            device_id={"cells": t * 2 + core},
            device_id_type=MESH,
        ).start()

    loop(chips - 1, spread_total)
    pltpu.make_async_copy(gs, gr.at[chip], recv_sem.at[5]).start()
    arrive(gr, 5)

    def join(t):
        wfin[pl.ds(t, 4, stride=chips), :] = gr[t]

    loop(chips, join, unroll=4)
    last = to_partner(wfin, wfin_r, 3)
    last.wait()

    def emit(low, high):
        gate_out[...] = low[0:width, :]
        out_out[...] = low[width : width + hidden, :]
        for e in range(2):
            proj_out[:, e * width : (e + 1) * width] = high[e * width : (e + 1) * width, :]

    low = jnp.where(core == 0, wfin[...], wfin_r[...])
    high = jnp.where(core == 0, wfin_r[...], wfin[...])
    emit(low, high)

    sent(s1, 0)
    sent(s2, 1)
    sent(s3, 2)
    sent(s4, 3)
    sent(ws, 4)
    view = gr.at[pl.ds(0, chips - 1)]
    pltpu.make_async_copy(view, view, send_sem.at[5]).wait()


def local(
    pair_act, pair_mask, chain_ids, proj_weight, gate_weight, chain_bias, out_weight, out_grad
):
    devices = lax.axis_size("cells")
    chips = devices // 2
    rows, length, width = pair_act.shape
    hidden = out_weight.shape[0]
    count = rows * length
    parts = length // LANES
    vm = pl.BlockSpec(memory_space=pltpu.VMEM)
    sm = pl.BlockSpec(memory_space=pltpu.SMEM)
    V = pltpu.VMEM
    eight, four = (chips, 8, length), (chips, 4, length)
    out = pl.pallas_call(
        kernel,
        out_shape=(
            jax.ShapeDtypeStruct((count, width), BF16),
            jax.ShapeDtypeStruct((width, 4 * hidden), F32),
            jax.ShapeDtypeStruct((width, width), F32),
            jax.ShapeDtypeStruct((hidden, width), F32),
        ),
        in_specs=[vm, vm, vm, vm, sm, vm, vm, vm, vm],
        out_specs=(vm, vm, vm, vm),
        scratch_shapes=[
            V((width, count), F32),
            V((1, count), F32),
            V((width, count), BF16),
            V((2 * hidden, count), F32),
            V((2 * hidden, count), F32),
            V((width, count), BF16),
            V((width, count), F32),
            V((hidden, count), F32),
            V((width, count), BF16),
            V((width, count), F32),
            V((hidden, count), BF16),
            V((4 * hidden, count), BF16),
            V((parts, 8 * chips, LANES), F32),
            V((parts, length, LANES), F32),
            V((parts, 4 * chips, LANES), F32),
            V((rows * chips, length), BF16),
            V((length, length), BF16),
            V((rows * chips, length), BF16),
            V(eight, BF16),
            V(eight, BF16),
            V(eight, BF16),
            V(four, BF16),
            V(four, BF16),
            V(four, BF16),
            V(four, BF16),
            V(eight, BF16),
            V(eight, BF16),
            V((parts, rows * chips, LANES), F32),
            V((parts, rows * chips, LANES), F32),
            V((4 * width, width), F32),
            V((4 * chips, width), F32),
            V((chips, 4, width), F32),
            V((chips, 4, width), F32),
            V((4, width), F32),
            V((chips, 4, width), F32),
            V((4 * chips, width), F32),
            V((4 * chips, width), F32),
            pltpu.SemaphoreType.DMA((6,)),
            pltpu.SemaphoreType.DMA((6,)),
            pltpu.SemaphoreType.DMA((4,)),
            pltpu.SemaphoreType.DMA((4,)),
        ],
        compiler_params=pltpu.CompilerParams(
            collective_id=0, has_side_effects=True, vmem_limit_bytes=60 * 1024 * 1024
        ),
    )(
        pair_act.reshape(count, width),
        out_grad.reshape(count, width),
        pair_mask.reshape(rows, 1, length),
        chain_ids.reshape(1, length),
        chain_ids,
        proj_weight,
        gate_weight,
        chain_bias.T,
        out_weight,
    )
    return (out[0].reshape(rows, length, width), out[1], out[2], out[3])


def solution(mesh):
    placed = (
        P(("groups", "cells"), None, None),
        P(("groups", "cells"), None),
        P("groups"),
        P(),
        P(),
        P(),
        P(),
        P(("groups", "cells"), None, None),
    )
    return jax.shard_map(
        local,
        mesh=mesh,
        in_specs=placed,
        out_specs=(
            P(("groups", "cells"), None, None),
            P("groups", None),
            P("groups", None),
            P("groups", None),
        ),
        check_vma=False,
    )
```

```python
import math

import jax
import jax.numpy as jnp
from jax import lax
from jax.experimental import pallas as pl
from jax.experimental.pallas import tpu as pltpu
from jax.sharding import PartitionSpec as P

EPS = 1e-05
MESH = pl.DeviceIdType.MESH
F32 = jnp.float32
BF16 = jnp.bfloat16
LANES = 128
NT = (((1,), (1,)), ((), ()))
TN = (((0,), (0,)), ((), ()))
NN = (((1,), (0,)), ((), ()))


def dot(a, b, dims):
    return lax.dot_general(a, b, dims, preferred_element_type=F32)


def loop(n, body, unroll=1):
    def step(i, carry):
        body(i)
        return carry

    lax.fori_loop(0, n, step, 0, unroll=unroll)


def kernel(
    act_ref,
    grad_ref,
    mask_ref,
    chain_ref,
    own_ref,
    proj_ref,
    gate_ref,
    bias_ref,
    outw_ref,
    pair_out,
    proj_out,
    gate_out,
    out_out,
    zhat_s,
    zscale_s,
    norm_s,
    p1_s,
    p2_s,
    do_s,
    e_s,
    dh_s,
    dl_s,
    dn_s,
    trilow_s,
    dproj_s,
    spread,
    wide,
    flat,
    a_s,
    b_s,
    dt_s,
    s1,
    r1,
    r1p,
    s2,
    r2,
    s3,
    r3,
    s4,
    r4,
    half_s,
    half_r,
    w1,
    line1,
    mid1a,
    column1,
    mid1b,
    full1,
    w2,
    line2,
    mid2a,
    column2,
    mid2b,
    full2,
    send_sem,
    recv_sem,
    pair_send,
    pair_recv,
    line_send,
    line_recv,
):
    me = lax.axis_index("cells")
    devices = lax.axis_size("cells")
    chips = devices // 2
    side = math.isqrt(chips)
    chip = me // 2
    core = lax.rem(me, 2)
    row, col = chip // side, lax.rem(chip, side)
    far = sorted(range(side), key=lambda d: -min(d, side - d))
    partner = me + 1 - 2 * core
    rows, length = mask_ref.shape
    width = act_ref.shape[1]
    hidden = outw_ref.shape[0]
    parts = length // LANES
    chunks = rows * parts
    tall = hidden // 8
    groups = chips // 8

    barrier = pltpu.get_barrier_semaphore()

    def each_chip(fn):
        def line(i):
            step = side // 2 + ((i + 1) // 2) * (1 - 2 * lax.rem(i, 2))
            base = lax.rem(row + step, side) * side
            for d in far:
                fn(base + lax.rem(col + d, side))

        loop(side - 1, line)
        for d in far[:-1]:
            fn(row * side + lax.rem(col + d, side))

    def greet(peer):
        pl.semaphore_signal(barrier, inc=1, device_id={"cells": peer}, device_id_type=MESH)

    each_chip(lambda t: greet(t * 2 + core))
    for d in far[:-1]:
        greet((row * side + lax.rem(col + d, side)) * 2 + 1 - core)
    greet(partner)

    def exchange(src, dst, k):
        def one(t):
            pltpu.make_async_remote_copy(
                src_ref=src.at[t],
                dst_ref=dst.at[chip],
                send_sem=send_sem.at[k],
                recv_sem=recv_sem.at[k],
                device_id={"cells": t * 2 + core},
                device_id_type=MESH,
            ).start()

        each_chip(one)
        pltpu.make_async_copy(src.at[chip], dst.at[chip], recv_sem.at[k]).start()

    def arrive(dst, k):
        pltpu.make_async_copy(dst, dst, recv_sem.at[k]).wait()

    def sent(src, k):
        view = src.at[pl.ds(0, chips - 1)]
        pltpu.make_async_copy(view, view, send_sem.at[k]).wait()

    def to_partner(src, dst, k):
        copy = pltpu.make_async_remote_copy(
            src_ref=src,
            dst_ref=dst,
            send_sem=pair_send.at[k],
            recv_sem=pair_recv.at[k],
            device_id={"cells": partner},
            device_id_type=MESH,
        )
        copy.start()
        return copy

    def cols(kq, r=0):
        return pl.ds(pl.multiple_of((r * parts + kq) * LANES, LANES), LANES)

    def cells(body, unroll=1):
        for r in range(rows):
            loop(parts, lambda kq, r=r: body(r, kq), unroll)

    def unpack(src, dst):
        n = src.shape[1]

        def one(t):
            at = pl.ds(pl.multiple_of(t * 8, 8), n)
            for kq in range(parts):
                dst[kq, at, :] = src[t, :, kq * LANES : (kq + 1) * LANES].astype(F32)

        loop(chips, one, unroll=4)

    def pack(src, dst):
        n = dst.shape[1]

        def one(t):
            at = pl.ds(pl.multiple_of(t * 8, 8), n)
            for kq in range(parts):
                dst[t, :, kq * LANES : (kq + 1) * LANES] = src[kq, at, :].astype(BF16)

        loop(chips, one, unroll=4)

    def pack_rows(src, dst, at):
        def one(t):
            for kq in range(parts):
                dst[t, at : at + 4, kq * LANES : (kq + 1) * LANES] = src[
                    kq, pl.ds(t, 4, stride=chips), :
                ].astype(BF16)

        loop(chips, one, unroll=4)

    def gather_rows(src, offset, dst):
        for r in range(rows):
            for g in range(0, groups, 2):
                for kq in range(parts):
                    both = [
                        src[kq, pl.ds((g + e) * 64 + offset + r, 8, stride=8), :] for e in range(2)
                    ]
                    dst[
                        r * chips + g * 8 : r * chips + g * 8 + 16, kq * LANES : (kq + 1) * LANES
                    ] = jnp.concatenate(both, axis=0).astype(BF16)

    eye = (
        lax.broadcasted_iota(jnp.int32, (width, width), 0)
        == lax.broadcasted_iota(jnp.int32, (width, width), 1)
    ).astype(BF16)

    def front(r, kq):
        q = cols(kq, r)
        z = dot(eye, act_ref[q, :], NT)
        center = z - jnp.mean(z, axis=0, keepdims=True)
        scale = lax.rsqrt(jnp.mean(center * center, axis=0, keepdims=True) + EPS)
        zhat = center * scale
        low = zhat.astype(BF16)
        zhat_s[:, q] = zhat
        zscale_s[:, q] = scale
        norm_s[:, q] = low
        projected = dot(proj_ref[...], low, TN)
        keeper = mask_ref[r : r + 1, cols(kq)].astype(F32)
        values = projected[: 2 * hidden]
        sigma = jax.nn.sigmoid(projected[2 * hidden :])
        p1 = keeper * sigma
        factors = p1 * values
        p1_s[:, q] = p1
        p2_s[:, q] = factors * (1.0 - sigma)
        for ab in range(2):
            for g in range(tall):
                at = ab * hidden + g * 8
                spread[kq, pl.ds(g * 64 + ab * 4 + r, 8, stride=8), :] = factors[at : at + 8]

    cells(front, unroll=3)
    pack(spread, s1)
    pl.semaphore_wait(barrier, chips + side - 1)
    exchange(s1, r1, 0)

    within, across = (
        jnp.sum(eye.astype(F32) * bias_ref[e : e + 1, :], axis=1, keepdims=True) for e in range(2)
    )
    def gating(r, kq):
        q = cols(kq, r)
        same = chain_ref[cols(kq)].reshape(1, LANES) == own_ref[me * rows + r]
        logits = dot(gate_ref[...], norm_s[:, q], TN)
        logits = logits + jnp.where(same, within, across)
        gate = jax.nn.sigmoid(logits)
        up = dot(eye, grad_ref[q, :], NT) * gate
        low = up.astype(BF16)
        do_s[:, q] = low
        e_s[:, q] = up * (1.0 - gate)
        dh_s[:, q] = dot(outw_ref[...], low, NN)

    cells(gating, unroll=3)

    arrive(r1, 0)
    first = to_partner(r1, r1p, 0)
    unpack(r1, spread)
    gather_rows(spread, 0, a_s)

    def place_right(src, which):
        for r in range(rows):
            for g in range(groups):
                for kq in range(parts):
                    wide[kq, pl.ds(g * 48 + 3 * which + r, 8, stride=6), :] = src[
                        kq, pl.ds(g * 64 + 4 + r, 8, stride=8), :
                    ]

    place_right(spread, core)
    first.wait()
    unpack(r1p, spread)
    place_right(spread, 1 - core)
    for kq in range(parts):
        b_s[:, kq * LANES : (kq + 1) * LANES] = wide[kq].astype(BF16)
    for kq in range(parts):
        flat[kq, : rows * chips, :] = dot(
            a_s[...], b_s[kq * LANES : (kq + 1) * LANES, :], NT
        )
    pack_rows(flat, s2, 0)
    exchange(s2, r2, 1)

    arrive(r2, 1)
    unpack(r2, spread)

    def middle(r, kq):
        q = cols(kq, r)
        tri = jnp.concatenate(
            [spread[kq, pl.ds(g * 64 + r, 8, stride=8), :] for g in range(tall)], axis=0
        )
        center = tri - jnp.mean(tri, axis=0, keepdims=True)
        scale = lax.rsqrt(jnp.mean(center * center, axis=0, keepdims=True) + EPS)
        hat = center * scale
        low = hat.astype(BF16)
        trilow_s[:, q] = low
        outputs = dot(outw_ref[...], low, TN)
        dl_s[:, q] = (outputs * e_s[:, q]).astype(BF16)
        d_hat = dh_s[:, q]
        m1 = jnp.mean(d_hat, axis=0, keepdims=True)
        m2 = jnp.mean(d_hat * hat, axis=0, keepdims=True)
        d_tri = scale * (d_hat - m1 - hat * m2)
        for g in range(tall):
            spread[kq, pl.ds(g * 64 + 4 + r, 8, stride=8), :] = d_tri[g * 8 : g * 8 + 8]

    cells(middle, unroll=3)

    def pack_upper(t):
        at = pl.ds(pl.multiple_of(t * 8, 8), 8)
        for kq in range(parts):
            s3[t, :, kq * LANES : (kq + 1) * LANES] = spread[kq, at, :][4:8].astype(BF16)

    loop(chips, pack_upper, unroll=4)
    exchange(s3, r3, 2)

    share = 2 * side
    spot = col * 2 + core
    block = w1.shape[0] // share

    def own(m):
        return pl.ds(pl.multiple_of(m * block, block), block)

    def line_peers(fn):
        for d in far:
            for e in range(2):
                if d or e:
                    fn((row * side + lax.rem(col + d, side)) * 2 + (1 - core if e else core))

    def send(src, dst, k, device):
        pltpu.make_async_remote_copy(
            src_ref=src,
            dst_ref=dst,
            send_sem=line_send.at[k],
            recv_sem=line_recv.at[k],
            device_id={"cells": device},
            device_id_type=MESH,
        ).start()

    def scatter_line(src, dst, k):
        line_peers(lambda p: send(src.at[own(lax.rem(p, share))], dst.at[spot], k, p))
        pltpu.make_async_copy(src.at[own(spot)], dst.at[spot], line_recv.at[k]).start()

    def reduce_column(src, mid, dst, k):
        pltpu.make_async_copy(src, src, line_recv.at[k - 1]).wait()
        mid[...] = jnp.sum(src[...].astype(F32), axis=0)
        for d in far[:-1]:
            p = (lax.rem(row + d, side) * side + col) * 2 + core
            send(mid, dst.at[row], k, p)
        pltpu.make_async_copy(mid, dst.at[row], line_recv.at[k]).start()

    def gather_line(src, mid, dst, k):
        pltpu.make_async_copy(src, src, line_recv.at[k - 1]).wait()
        mid[...] = jnp.sum(src[...], axis=0) * (1.0 / length)
        line_peers(lambda p: send(mid, dst.at[own(spot)], k, p))
        pltpu.make_async_copy(mid, dst.at[own(spot)], line_recv.at[k]).start()

    def drain(w, mid, dst, k):
        view = w.at[pl.ds(0, (share - 1) * block)]
        pltpu.make_async_copy(view, view, line_send.at[k]).wait()
        view = dst.at[pl.ds(0, (side - 1) * block)]
        pltpu.make_async_copy(view, view, line_send.at[k + 1]).wait()
        view = dst.at[pl.ds(0, (share - 1) * block)]
        pltpu.make_async_copy(view, view, line_send.at[k + 2]).wait()

    w1[0:width, :] = dot(norm_s[...], dl_s[...], NT).astype(BF16)
    w1[width : width + hidden, :] = dot(trilow_s[...], do_s[...], NT).astype(BF16)
    w1[width + hidden : 2 * width, :] = jnp.zeros((width - hidden, width), BF16)
    scatter_line(w1, line1, 0)

    def gate_part(r, kq):
        q = cols(kq, r)
        dn_s[:, q] = dot(gate_ref[...], dl_s[:, q], NN)

    cells(gate_part, unroll=3)

    arrive(r3, 2)
    unpack(r3, spread)
    gather_rows(spread, 0, dt_s)
    for kq in range(parts):
        wide[kq] = dot(dt_s[...], a_s[:, kq * LANES : (kq + 1) * LANES], TN)
    for r in range(rows):
        for g in range(groups):
            for kq in range(parts):
                half_s[kq, r * chips + g * 8 : r * chips + g * 8 + 8, :] = wide[
                    kq, pl.ds(g * 48 + 3 * (1 - core) + r, 8, stride=6), :
                ]
    second = to_partner(half_s, half_r, 1)
    for kq in range(parts):
        flat[kq, : rows * chips, :] = dot(
            dt_s[...], b_s[:, kq * LANES : (kq + 1) * LANES], NN
        )
    pack_rows(flat, s4, 0)
    second.wait()
    for r in range(rows):
        for g in range(groups):
            for kq in range(parts):
                at = slice(r * chips + g * 8, r * chips + g * 8 + 8)
                flat[kq, at, :] = (
                    wide[kq, pl.ds(g * 48 + 3 * core + r, 8, stride=6), :] + half_r[kq, at, :]
                )
    pack_rows(flat, s4, 4)
    exchange(s4, r4, 3)
    reduce_column(line1, mid1a, column1, 1)

    arrive(r4, 3)
    unpack(r4, spread)

    def factor_back(r, kq):
        q = cols(kq, r)
        d_factors = jnp.concatenate(
            [
                spread[kq, pl.ds(g * 64 + ab * 4 + r, 8, stride=8), :]
                for ab in range(2)
                for g in range(tall)
            ],
            axis=0,
        )
        dproj_s[: 2 * hidden, q] = (d_factors * p1_s[:, q]).astype(BF16)
        dproj_s[2 * hidden :, q] = (d_factors * p2_s[:, q]).astype(BF16)

    cells(factor_back, unroll=3)
    for e in range(2):
        w2[e * width : (e + 1) * width, :] = dot(
            norm_s[...], dproj_s[e * width : (e + 1) * width, :], NT
        ).astype(BF16)
    scatter_line(w2, line2, 3)
    gather_line(column1, mid1b, full1, 2)

    def finish(r, kq):
        q = cols(kq, r)
        d_norm = dot(proj_ref[...], dproj_s[:, q], NN) + dn_s[:, q]
        zhat = zhat_s[:, q]
        m1 = jnp.mean(d_norm, axis=0, keepdims=True)
        m2 = jnp.mean(d_norm * zhat, axis=0, keepdims=True)
        grad = zscale_s[:, q] * (d_norm - m1 - zhat * m2)
        pair_out[q, :] = grad.T.astype(BF16)

    cells(finish, unroll=3)
    reduce_column(line2, mid2a, column2, 4)
    gather_line(column2, mid2b, full2, 5)
    pltpu.make_async_copy(full1, full1, line_recv.at[2]).wait()
    gate_out[...] = full1[0:width, :]
    out_out[...] = full1[width : width + hidden, :]
    sent(s1, 0)
    sent(s2, 1)
    sent(s3, 2)
    sent(s4, 3)
    drain(w1, mid1b, full1, 0)
    pltpu.make_async_copy(full2, full2, line_recv.at[5]).wait()
    for e in range(2):
        proj_out[:, e * width : (e + 1) * width] = full2[e * width : (e + 1) * width, :]
    drain(w2, mid2b, full2, 3)


def local(
    pair_act, pair_mask, chain_ids, proj_weight, gate_weight, chain_bias, out_weight, out_grad
):
    devices = lax.axis_size("cells")
    chips = devices // 2
    rows, length, width = pair_act.shape
    hidden = out_weight.shape[0]
    count = rows * length
    parts = length // LANES
    side = math.isqrt(chips)
    share = 2 * side
    block = 2 * width // share
    vm = pl.BlockSpec(memory_space=pltpu.VMEM)
    sm = pl.BlockSpec(memory_space=pltpu.SMEM)
    V = pltpu.VMEM
    eight, four = (chips, 8, length), (chips, 4, length)
    out = pl.pallas_call(
        kernel,
        out_shape=(
            jax.ShapeDtypeStruct((count, width), BF16),
            jax.ShapeDtypeStruct((width, 4 * hidden), F32),
            jax.ShapeDtypeStruct((width, width), F32),
            jax.ShapeDtypeStruct((hidden, width), F32),
        ),
        in_specs=[vm, vm, vm, vm, sm, vm, vm, vm, vm],
        out_specs=(vm, vm, vm, vm),
        scratch_shapes=[
            V((width, count), F32),
            V((1, count), F32),
            V((width, count), BF16),
            V((2 * hidden, count), F32),
            V((2 * hidden, count), F32),
            V((width, count), BF16),
            V((width, count), F32),
            V((hidden, count), F32),
            V((width, count), BF16),
            V((width, count), F32),
            V((hidden, count), BF16),
            V((4 * hidden, count), BF16),
            V((parts, 8 * chips, LANES), F32),
            V((parts, length, LANES), F32),
            V((parts, 4 * chips, LANES), F32),
            V((rows * chips, length), BF16),
            V((length, length), BF16),
            V((rows * chips, length), BF16),
            V(eight, BF16),
            V(eight, BF16),
            V(eight, BF16),
            V(four, BF16),
            V(four, BF16),
            V(four, BF16),
            V(four, BF16),
            V(eight, BF16),
            V(eight, BF16),
            V((parts, rows * chips, LANES), F32),
            V((parts, rows * chips, LANES), F32),
            *(2 * [
                V((2 * width, width), BF16),
                V((share, block, width), BF16),
                V((block, width), F32),
                V((side, block, width), F32),
                V((block, width), F32),
                V((2 * width, width), F32),
            ]),
            pltpu.SemaphoreType.DMA((4,)),
            pltpu.SemaphoreType.DMA((4,)),
            pltpu.SemaphoreType.DMA((2,)),
            pltpu.SemaphoreType.DMA((2,)),
            pltpu.SemaphoreType.DMA((6,)),
            pltpu.SemaphoreType.DMA((6,)),
        ],
        compiler_params=pltpu.CompilerParams(
            collective_id=0, has_side_effects=True, vmem_limit_bytes=20 * 1024 * 1024
        ),
    )(
        pair_act.reshape(count, width),
        out_grad.reshape(count, width),
        pair_mask,
        chain_ids,
        chain_ids,
        proj_weight,
        gate_weight,
        chain_bias,
        out_weight,
    )
    return (out[0].reshape(rows, length, width), out[1], out[2], out[3])


def solution(mesh):
    placed = (
        P(("groups", "cells"), None, None),
        P(("groups", "cells"), None),
        P("groups"),
        P(),
        P(),
        P(),
        P(),
        P(("groups", "cells"), None, None),
    )
    return jax.shard_map(
        local,
        mesh=mesh,
        in_specs=placed,
        out_specs=(
            P(("groups", "cells"), None, None),
            P("groups", None),
            P("groups", None),
            P("groups", None),
        ),
        check_vma=False,
    )
```

```python
import math

import jax
import jax.numpy as jnp
from jax import lax
from jax.experimental import pallas as pl
from jax.experimental.pallas import tpu as pltpu
from jax.sharding import PartitionSpec as P

EPS = 1e-05
MESH = pl.DeviceIdType.MESH
F32 = jnp.float32
BF16 = jnp.bfloat16
LANES = 128
NT = (((1,), (1,)), ((), ()))
TN = (((0,), (0,)), ((), ()))
NN = (((1,), (0,)), ((), ()))


def dot(a, b, dims):
    return lax.dot_general(a, b, dims, preferred_element_type=F32)


def loop(n, body, unroll=1):
    def step(i, carry):
        body(i)
        return carry

    lax.fori_loop(0, n, step, 0, unroll=unroll)


def kernel(
    act_hbm,
    grad_hbm,
    mask_hbm,
    chain_hbm,
    proj_hbm,
    gate_hbm,
    bias_hbm,
    outw_hbm,
    pair_out,
    proj_out,
    gate_out,
    out_out,
    act_ref,
    grad_ref,
    mask_ref,
    chain_ref,
    own_ref,
    proj_ref,
    gate_ref,
    bias_ref,
    outw_ref,
    in_sem,
    zhat_s,
    zscale_s,
    norm_s,
    p1_s,
    p2_s,
    do_s,
    e_s,
    dh_s,
    dl_s,
    dn_s,
    trilow_s,
    dproj_s,
    spread,
    wide,
    flat,
    a_s,
    b_s,
    dt_s,
    spread2,
    s1a,
    s1b,
    s2,
    s3,
    s4a,
    s4b,
    r1a,
    r1b,
    r1p,
    r2,
    r3,
    r4a,
    r4b,
    half_s,
    half_r,
    w1,
    line1,
    mid1a,
    column1,
    mid1b,
    full1,
    w2,
    line2,
    mid2a,
    column2,
    mid2b,
    full2,
    w3,
    line3,
    mid3a,
    column3,
    mid3b,
    full3,
    send_sem,
    recv_sem,
    pair_send,
    pair_recv,
    line_send,
    line_recv,
):
    loads = [
        pltpu.make_async_copy(src, dst, in_sem.at[k])
        for k, (src, dst) in enumerate(
            (
                (act_hbm, act_ref),
                (proj_hbm, proj_ref),
                (mask_hbm, mask_ref),
                (grad_hbm, grad_ref),
                (gate_hbm, gate_ref),
                (outw_hbm, outw_ref),
                (bias_hbm, bias_ref),
                (chain_hbm, chain_ref),
                (chain_hbm, own_ref),
            )
        )
    ]
    for load in loads:
        load.start()
    me = lax.axis_index("cells")
    devices = lax.axis_size("cells")
    chips = devices // 2
    side = math.isqrt(chips)
    chip = me // 2
    core = lax.rem(me, 2)
    row, col = chip // side, lax.rem(chip, side)
    far = sorted(range(side), key=lambda d: -min(d, side - d))
    partner = me + 1 - 2 * core
    rows, length = mask_ref.shape
    width = act_ref.shape[1]
    hidden = outw_ref.shape[0]
    parts = length // LANES
    tall = hidden // 8
    groups = chips // 8

    barrier = pltpu.get_barrier_semaphore()

    def each_chip(fn):
        def line(i):
            step = side // 2 + ((i + 1) // 2) * (1 - 2 * lax.rem(i, 2))
            base = lax.rem(row + step, side) * side
            for d in far:
                fn(base + lax.rem(col + d, side))

        loop(side - 1, line)
        for d in far[:-1]:
            fn(row * side + lax.rem(col + d, side))

    def greet(peer):
        pl.semaphore_signal(barrier, inc=1, device_id={"cells": peer}, device_id_type=MESH)

    each_chip(lambda t: greet(t * 2 + core))
    for d in far[:-1]:
        greet((row * side + lax.rem(col + d, side)) * 2 + 1 - core)
    greet(partner)

    def exchange(src, dst, k):
        def one(t):
            pltpu.make_async_remote_copy(
                src_ref=src.at[t],
                dst_ref=dst.at[chip],
                send_sem=send_sem.at[k],
                recv_sem=recv_sem.at[k],
                device_id={"cells": t * 2 + core},
                device_id_type=MESH,
            ).start()

        each_chip(one)
        pltpu.make_async_copy(src.at[chip], dst.at[chip], recv_sem.at[k]).start()

    def arrive(dst, k):
        pltpu.make_async_copy(dst, dst, recv_sem.at[k]).wait()

    def sent(src, k):
        view = src.at[pl.ds(0, chips - 1)]
        pltpu.make_async_copy(view, view, send_sem.at[k]).wait()

    def to_partner(src, dst, k):
        copy = pltpu.make_async_remote_copy(
            src_ref=src,
            dst_ref=dst,
            send_sem=pair_send.at[k],
            recv_sem=pair_recv.at[k],
            device_id={"cells": partner},
            device_id_type=MESH,
        )
        copy.start()
        return copy

    def cols(kq, r=0):
        return pl.ds(pl.multiple_of((r * parts + kq) * LANES, LANES), LANES)

    def cells(body, unroll=1):
        for r in range(rows):
            loop(parts, lambda kq, r=r: body(r, kq), unroll)

    def unpack(src, dst):
        n = src.shape[1]

        def one(t):
            at = pl.ds(pl.multiple_of(t * 8, 8), n)
            for kq in range(parts):
                dst[kq, at, :] = src[t, :, kq * LANES : (kq + 1) * LANES].astype(F32)

        loop(chips, one, unroll=4)

    def pack(src, dst):
        n = dst.shape[1]

        def one(t):
            at = pl.ds(pl.multiple_of(t * 8, 8), n)
            for kq in range(parts):
                dst[t, :, kq * LANES : (kq + 1) * LANES] = src[kq, at, :].astype(BF16)

        loop(chips, one, unroll=4)

    def pack_rows(src, dst):
        def one(t):
            for kq in range(parts):
                dst[t, :, kq * LANES : (kq + 1) * LANES] = src[
                    kq, pl.ds(t, 4, stride=chips), :
                ].astype(BF16)

        loop(chips, one, unroll=4)

    def gather_rows(src, offset, dst):
        for r in range(rows):
            for g in range(0, groups, 2):
                for kq in range(parts):
                    both = [
                        src[kq, pl.ds((g + e) * 64 + offset + r, 8, stride=8), :] for e in range(2)
                    ]
                    dst[
                        r * chips + g * 8 : r * chips + g * 8 + 16, kq * LANES : (kq + 1) * LANES
                    ] = jnp.concatenate(both, axis=0).astype(BF16)

    eye = (
        lax.broadcasted_iota(jnp.int32, (width, width), 0)
        == lax.broadcasted_iota(jnp.int32, (width, width), 1)
    ).astype(BF16)

    for load in loads[:3]:
        load.wait()

    def front(r, kq):
        q = cols(kq, r)
        z = dot(eye, act_ref[q, :], NT)
        center = z - jnp.mean(z, axis=0, keepdims=True)
        scale = lax.rsqrt(jnp.mean(center * center, axis=0, keepdims=True) + EPS)
        zhat = center * scale
        low = zhat.astype(BF16)
        zhat_s[:, q] = zhat
        zscale_s[:, q] = scale
        norm_s[:, q] = low
        projected = dot(proj_ref[...], low, TN)
        keeper = mask_ref[r : r + 1, cols(kq)].astype(F32)
        values = projected[: 2 * hidden]
        sigma = jax.nn.sigmoid(projected[2 * hidden :])
        p1 = keeper * sigma
        factors = p1 * values
        p1_s[:, q] = p1
        p2_s[:, q] = factors * (1.0 - sigma)
        for ab in range(2):
            for g in range(tall):
                at = ab * hidden + g * 8
                (spread, spread2)[ab][kq, pl.ds(g * 64 + r, 8, stride=8), :] = factors[at : at + 8]

    cells(front, unroll=3)
    pack(spread2, s1b)
    pack(spread, s1a)
    pl.semaphore_wait(barrier, chips + side - 1)
    exchange(s1b, r1b, 0)
    exchange(s1a, r1a, 1)

    for load in loads[3:]:
        load.wait()
    within, across = (
        jnp.sum(eye.astype(F32) * bias_ref[e : e + 1, :], axis=1, keepdims=True) for e in range(2)
    )
    def gating(r, kq):
        q = cols(kq, r)
        same = chain_ref[cols(kq)].reshape(1, LANES) == own_ref[me * rows + r]
        logits = dot(gate_ref[...], norm_s[:, q], TN)
        logits = logits + jnp.where(same, within, across)
        gate = jax.nn.sigmoid(logits)
        up = dot(eye, grad_ref[q, :], NT) * gate
        low = up.astype(BF16)
        do_s[:, q] = low
        e_s[:, q] = up * (1.0 - gate)
        dh_s[:, q] = dot(outw_ref[...], low, NN)

    cells(gating, unroll=3)

    arrive(r1b, 0)
    first = to_partner(r1b, r1p, 0)
    unpack(r1b, spread2)

    def place_right(src, which):
        for r in range(rows):
            for g in range(groups):
                for kq in range(parts):
                    wide[kq, pl.ds(g * 48 + 3 * which + r, 8, stride=6), :] = src[
                        kq, pl.ds(g * 64 + r, 8, stride=8), :
                    ]

    place_right(spread2, core)
    first.wait()
    unpack(r1p, spread2)
    place_right(spread2, 1 - core)
    arrive(r1a, 1)
    unpack(r1a, spread)
    gather_rows(spread, 0, a_s)
    for kq in range(parts):
        b_s[:, kq * LANES : (kq + 1) * LANES] = wide[kq].astype(BF16)
    for kq in range(parts):
        flat[kq, : rows * chips, :] = dot(
            a_s[...], b_s[kq * LANES : (kq + 1) * LANES, :], NT
        )
    pack_rows(flat, s2)
    exchange(s2, r2, 2)

    arrive(r2, 2)
    unpack(r2, spread)

    def middle(r, kq):
        q = cols(kq, r)
        tri = jnp.concatenate(
            [spread[kq, pl.ds(g * 64 + r, 8, stride=8), :] for g in range(tall)], axis=0
        )
        center = tri - jnp.mean(tri, axis=0, keepdims=True)
        scale = lax.rsqrt(jnp.mean(center * center, axis=0, keepdims=True) + EPS)
        hat = center * scale
        low = hat.astype(BF16)
        trilow_s[:, q] = low
        outputs = dot(outw_ref[...], low, TN)
        dl_s[:, q] = (outputs * e_s[:, q]).astype(BF16)
        d_hat = dh_s[:, q]
        m1 = jnp.mean(d_hat, axis=0, keepdims=True)
        m2 = jnp.mean(d_hat * hat, axis=0, keepdims=True)
        d_tri = scale * (d_hat - m1 - hat * m2)
        for g in range(tall):
            spread2[kq, pl.ds(g * 64 + r, 8, stride=8), :] = d_tri[g * 8 : g * 8 + 8]

    cells(middle, unroll=3)

    pack(spread2, s3)
    exchange(s3, r3, 3)

    share = 2 * side
    spot = col * 2 + core

    def put(w, value):
        n = w.shape[1]
        for m in range(share):
            w[m] = value[m * n : (m + 1) * n].astype(BF16)

    def line_peers(fn):
        for d in far:
            for e in range(2):
                if d or e:
                    fn((row * side + lax.rem(col + d, side)) * 2 + (1 - core if e else core))

    def send(src, dst, k, device):
        pltpu.make_async_remote_copy(
            src_ref=src,
            dst_ref=dst,
            send_sem=line_send.at[k],
            recv_sem=line_recv.at[k],
            device_id={"cells": device},
            device_id_type=MESH,
        ).start()

    def scatter_line(src, dst, k):
        line_peers(lambda p: send(src.at[lax.rem(p, share)], dst.at[spot], k, p))
        pltpu.make_async_copy(src.at[spot], dst.at[spot], line_recv.at[k]).start()

    def reduce_column(src, mid, dst, k):
        pltpu.make_async_copy(src, src, line_recv.at[k - 1]).wait()
        mid[...] = jnp.sum(src[...].astype(F32), axis=0)
        for d in far[:-1]:
            p = (lax.rem(row + d, side) * side + col) * 2 + core
            send(mid, dst.at[row], k, p)
        pltpu.make_async_copy(mid, dst.at[row], line_recv.at[k]).start()

    def gather_line(src, mid, dst, k):
        pltpu.make_async_copy(src, src, line_recv.at[k - 1]).wait()
        mid[...] = (jnp.sum(src[...], axis=0) * (1.0 / length)).astype(BF16)
        line_peers(lambda p: send(mid, dst.at[spot], k, p))
        pltpu.make_async_copy(mid, dst.at[spot], line_recv.at[k]).start()

    def drain(w, column, full, k):
        for e, (src, n) in enumerate(((w, share), (column, side), (full, share))):
            view = src.at[pl.ds(0, n - 1)]
            pltpu.make_async_copy(view, view, line_send.at[k + e]).wait()

    put(
        w1,
        jnp.concatenate(
            [
                dot(norm_s[...], dl_s[...], NT),
                dot(trilow_s[...], do_s[...], NT),
                jnp.zeros((width - hidden, width), F32),
            ],
            axis=0,
        ),
    )
    scatter_line(w1, line1, 0)

    def gate_part(r, kq):
        q = cols(kq, r)
        dn_s[:, q] = dot(gate_ref[...], dl_s[:, q], NN)

    cells(gate_part, unroll=3)

    arrive(r3, 3)
    unpack(r3, spread)
    gather_rows(spread, 0, dt_s)
    for kq in range(parts):
        wide[kq] = dot(dt_s[...], a_s[:, kq * LANES : (kq + 1) * LANES], TN)
    for r in range(rows):
        for g in range(groups):
            for kq in range(parts):
                half_s[kq, r * chips + g * 8 : r * chips + g * 8 + 8, :] = wide[
                    kq, pl.ds(g * 48 + 3 * (1 - core) + r, 8, stride=6), :
                ]
    second = to_partner(half_s, half_r, 1)
    for kq in range(parts):
        flat[kq, : rows * chips, :] = dot(
            dt_s[...], b_s[:, kq * LANES : (kq + 1) * LANES], NN
        )
    pack_rows(flat, s4a)
    exchange(s4a, r4a, 4)
    second.wait()
    for r in range(rows):
        for g in range(groups):
            for kq in range(parts):
                at = slice(r * chips + g * 8, r * chips + g * 8 + 8)
                flat[kq, at, :] = (
                    wide[kq, pl.ds(g * 48 + 3 * core + r, 8, stride=6), :] + half_r[kq, at, :]
                )
    pack_rows(flat, s4b)
    exchange(s4b, r4b, 5)
    reduce_column(line1, mid1a, column1, 1)

    def half_back(ab, src, k, w, line, base):
        arrive(src, k)
        unpack(src, spread)
        at = slice(ab * hidden, (ab + 1) * hidden)
        up = slice((2 + ab) * hidden, (3 + ab) * hidden)

        def factor_back(r, kq):
            q = cols(kq, r)
            d_factors = jnp.concatenate(
                [spread[kq, pl.ds(g * 64 + r, 8, stride=8), :] for g in range(tall)], axis=0
            )
            dproj_s[at, q] = (d_factors * p1_s[at, q]).astype(BF16)
            dproj_s[up, q] = (d_factors * p2_s[at, q]).astype(BF16)

        cells(factor_back, unroll=3)
        put(
            w,
            dot(norm_s[...], jnp.concatenate([dproj_s[at, :], dproj_s[up, :]], axis=0), NT),
        )
        scatter_line(w, line, base)

    half_back(0, r4a, 4, w2, line2, 3)
    gather_line(column1, mid1b, full1, 2)
    half_back(1, r4b, 5, w3, line3, 6)

    def finish(r, kq):
        q = cols(kq, r)
        d_norm = dot(proj_ref[...], dproj_s[:, q], NN) + dn_s[:, q]
        zhat = zhat_s[:, q]
        m1 = jnp.mean(d_norm, axis=0, keepdims=True)
        m2 = jnp.mean(d_norm * zhat, axis=0, keepdims=True)
        grad = zscale_s[:, q] * (d_norm - m1 - zhat * m2)
        pair_out[q, :] = grad.T.astype(BF16)

    reduce_column(line2, mid2a, column2, 4)
    cells(finish, unroll=3)
    reduce_column(line3, mid3a, column3, 7)
    gather_line(column2, mid2b, full2, 5)

    def landed(full, k):
        pltpu.make_async_copy(full, full, line_recv.at[k]).wait()
        return full[...].astype(F32).reshape(full.shape[0] * full.shape[1], width)

    gather_line(column3, mid3b, full3, 8)
    sums = landed(full1, 2)
    gate_out[...] = sums[0:width]
    out_out[...] = sums[width : width + hidden]
    for k, src in enumerate((s1b, s1a, s2, s3, s4a, s4b)):
        sent(src, k)
    drain(w1, column1, full1, 0)
    drain(w2, column2, full2, 3)
    left, right = landed(full2, 5), landed(full3, 8)
    lower = lax.broadcasted_iota(jnp.int32, left.shape, 1) < hidden
    proj_out[:, 0:width] = jnp.where(lower, left, pltpu.roll(right, hidden, 1))
    proj_out[:, width : 2 * width] = jnp.where(lower, pltpu.roll(left, hidden, 1), right)
    drain(w3, column3, full3, 6)


def write(a_ref, b_ref, c_ref, d_ref, a_out, b_out, c_out, d_out, sem):
    copies = [
        pltpu.make_async_copy(src, dst, sem.at[k])
        for k, (src, dst) in enumerate(
            ((a_ref, a_out), (b_ref, b_out), (c_ref, c_out), (d_ref, d_out))
        )
    ]
    for copy in copies:
        copy.start()
    for copy in copies:
        copy.wait()


def local(
    pair_act, pair_mask, chain_ids, proj_weight, gate_weight, chain_bias, out_weight, out_grad
):
    devices = lax.axis_size("cells")
    chips = devices // 2
    rows, length, width = pair_act.shape
    hidden = out_weight.shape[0]
    count = rows * length
    parts = length // LANES
    side = math.isqrt(chips)
    share = 2 * side
    vm = pl.BlockSpec(memory_space=pltpu.VMEM)
    hbm = pl.BlockSpec(memory_space=pltpu.HBM)
    V = pltpu.VMEM
    four = (chips, 4, length)

    def reduction(block):
        return [
            V((share, block, width), BF16),
            V((share, block, width), BF16),
            V((block, width), F32),
            V((side, block, width), F32),
            V((block, width), BF16),
            V((share, block, width), BF16),
        ]

    shapes = (
        jax.ShapeDtypeStruct((count, width), BF16),
        jax.ShapeDtypeStruct((width, 4 * hidden), F32),
        jax.ShapeDtypeStruct((width, width), F32),
        jax.ShapeDtypeStruct((hidden, width), F32),
    )
    out = pl.pallas_call(
        kernel,
        out_shape=shapes,
        in_specs=8 * [hbm],
        out_specs=(vm, vm, vm, vm),
        scratch_shapes=[
            V((count, width), BF16),
            V((count, width), BF16),
            V((rows, length), jnp.int32),
            V((length,), jnp.int32),
            pltpu.SMEM((length,), jnp.int32),
            V((width, 4 * hidden), BF16),
            V((width, width), BF16),
            V((2, width), F32),
            V((hidden, width), BF16),
            pltpu.SemaphoreType.DMA((9,)),
            V((width, count), F32),
            V((1, count), F32),
            V((width, count), BF16),
            V((2 * hidden, count), F32),
            V((2 * hidden, count), F32),
            V((width, count), BF16),
            V((width, count), F32),
            V((hidden, count), F32),
            V((width, count), BF16),
            V((width, count), F32),
            V((hidden, count), BF16),
            V((4 * hidden, count), BF16),
            V((parts, 8 * chips, LANES), F32),
            V((parts, length, LANES), F32),
            V((parts, 4 * chips, LANES), F32),
            V((rows * chips, length), BF16),
            V((length, length), BF16),
            V((rows * chips, length), BF16),
            V((parts, 8 * chips, LANES), F32),
            *(13 * [V(four, BF16)]),
            V((parts, rows * chips, LANES), F32),
            V((parts, rows * chips, LANES), F32),
            *reduction(2 * width // share),
            *reduction(width // share),
            *reduction(width // share),
            pltpu.SemaphoreType.DMA((6,)),
            pltpu.SemaphoreType.DMA((6,)),
            pltpu.SemaphoreType.DMA((2,)),
            pltpu.SemaphoreType.DMA((2,)),
            pltpu.SemaphoreType.DMA((9,)),
            pltpu.SemaphoreType.DMA((9,)),
        ],
        compiler_params=pltpu.CompilerParams(
            collective_id=0, has_side_effects=True, vmem_limit_bytes=20 * 1024 * 1024
        ),
    )(
        *(
            pltpu.with_memory_space_constraint(x, pltpu.HBM)
            for x in (
                pair_act.reshape(count, width),
                out_grad.reshape(count, width),
                pair_mask,
                chain_ids,
                proj_weight,
                gate_weight,
                chain_bias,
                out_weight,
            )
        )
    )
    out = pl.pallas_call(
        write,
        out_shape=shapes,
        in_specs=4 * [vm],
        out_specs=tuple(4 * [hbm]),
        scratch_shapes=[pltpu.SemaphoreType.DMA((4,))],
        compiler_params=pltpu.CompilerParams(vmem_limit_bytes=4 * 1024 * 1024),
    )(*out)
    return (out[0].reshape(rows, length, width), out[1], out[2], out[3])


def solution(mesh):
    placed = (
        P(("groups", "cells"), None, None),
        P(("groups", "cells"), None),
        P("groups"),
        P(),
        P(),
        P(),
        P(),
        P(("groups", "cells"), None, None),
    )
    return jax.shard_map(
        local,
        mesh=mesh,
        in_specs=placed,
        out_specs=(
            P(("groups", "cells"), None, None),
            P("groups", None),
            P("groups", None),
            P("groups", None),
        ),
        check_vma=False,
    )
```

```python
import math

import jax
import jax.numpy as jnp
from jax import lax
from jax.experimental import pallas as pl
from jax.experimental.pallas import tpu as pltpu
from jax.sharding import PartitionSpec as P

EPS = 1e-05
MESH = pl.DeviceIdType.MESH
F32 = jnp.float32
BF16 = jnp.bfloat16
LANES = 128
SLOT = 24
NT = (((1,), (1,)), ((), ()))
TN = (((0,), (0,)), ((), ()))
NN = (((1,), (0,)), ((), ()))


def dot(a, b, dims):
    return lax.dot_general(a, b, dims, preferred_element_type=F32)


def loop(n, body, unroll=1):
    def step(i, carry):
        body(i)
        return carry

    lax.fori_loop(0, n, step, 0, unroll=unroll)


def kernel(
    act_hbm,
    grad_hbm,
    mask_hbm,
    chain_hbm,
    proj_hbm,
    gate_hbm,
    bias_hbm,
    outw_hbm,
    pair_out,
    proj_out,
    gate_out,
    out_out,
    act_ref,
    grad_ref,
    mask_ref,
    chain_ref,
    own_ref,
    proj_ref,
    gate_ref,
    bias_ref,
    outw_ref,
    in_sem,
    zhat_s,
    zscale_s,
    norm_s,
    p1_s,
    p2_s,
    do_s,
    e_s,
    dh_s,
    dl_s,
    dn_s,
    trilow_s,
    dproj_s,
    spread,
    wide,
    flat,
    a_s,
    b_s,
    dt_s,
    spread2,
    s1a,
    s1b,
    s2,
    s3,
    s4a,
    s4b,
    r1a,
    r1b,
    r1p,
    r2,
    r3,
    r4a,
    r4b,
    half_s,
    half_r,
    w1,
    line1,
    mid1a,
    column1,
    mid1b,
    full1,
    w2,
    line2,
    mid2a,
    column2,
    mid2b,
    full2,
    w3,
    line3,
    mid3a,
    column3,
    mid3b,
    full3,
    send_sem,
    recv_sem,
    pair_send,
    pair_recv,
    line_send,
    line_recv,
):
    loads = [
        pltpu.make_async_copy(src, dst, in_sem.at[k])
        for k, (src, dst) in enumerate(
            (
                (act_hbm, act_ref),
                (proj_hbm, proj_ref),
                (mask_hbm, mask_ref),
                (grad_hbm, grad_ref),
                (gate_hbm, gate_ref),
                (outw_hbm, outw_ref),
                (bias_hbm, bias_ref),
                (chain_hbm, chain_ref),
                (chain_hbm, own_ref),
            )
        )
    ]
    for load in loads:
        load.start()
    me = lax.axis_index("cells")
    devices = lax.axis_size("cells")
    chips = devices // 2
    side = math.isqrt(chips)
    chip = me // 2
    core = lax.rem(me, 2)
    row, col = chip // side, lax.rem(chip, side)
    far = sorted(range(side), key=lambda d: -min(d, side - d))
    partner = me + 1 - 2 * core
    rows, length = mask_ref.shape
    width = act_ref.shape[1]
    hidden = outw_ref.shape[0]
    parts = length // LANES
    tall = hidden // 8
    groups = chips // 8
    pairs = (rows * parts + 1) // 2

    barrier = pltpu.get_barrier_semaphore()

    def base_of(i):
        step = side // 2 + ((i + 1) // 2) * (1 - 2 * lax.rem(i, 2))
        return lax.rem(row + step, side) * side

    def each_chip(fn, prepare=None):
        def line(i):
            base, later = base_of(i), base_of(i + 1)
            for k, d in enumerate(far):
                if prepare is not None:
                    prepare(later + k)
                fn(base + lax.rem(col + d, side))

        if prepare is not None:
            for k in range(side):
                prepare(base_of(jnp.int32(0)) + k)
        loop(side - 1, line)
        for d in far[:-1]:
            fn(row * side + lax.rem(col + d, side))

    def greet(peer):
        pl.semaphore_signal(barrier, inc=1, device_id={"cells": peer}, device_id_type=MESH)

    each_chip(lambda t: greet(t * 2 + core))
    for d in far[:-1]:
        greet((row * side + lax.rem(col + d, side)) * 2 + 1 - core)
    greet(partner)

    def exchange(src, dst, k, prepare=None):
        def one(t):
            pltpu.make_async_remote_copy(
                src_ref=src.at[t],
                dst_ref=dst.at[chip],
                send_sem=send_sem.at[k],
                recv_sem=recv_sem.at[k],
                device_id={"cells": t * 2 + core},
                device_id_type=MESH,
            ).start()

        each_chip(one, prepare)
        pltpu.make_async_copy(src.at[chip], dst.at[chip], recv_sem.at[k]).start()

    def arrive(dst, k):
        pltpu.make_async_copy(dst, dst, recv_sem.at[k]).wait()

    def sent(src, k):
        view = src.at[pl.ds(0, chips - 1)]
        pltpu.make_async_copy(view, view, send_sem.at[k]).wait()

    def to_partner(src, dst, k):
        copy = pltpu.make_async_remote_copy(
            src_ref=src,
            dst_ref=dst,
            send_sem=pair_send.at[k],
            recv_sem=pair_recv.at[k],
            device_id={"cells": partner},
            device_id_type=MESH,
        )
        copy.start()
        return copy

    def cols(kq, r=0):
        return pl.ds(pl.multiple_of((r * parts + kq) * LANES, LANES), LANES)

    def cells(body, unroll=1):
        for r in range(rows):
            loop(parts, lambda kq, r=r: body(r, kq), unroll)

    def unpack(src, dst):
        def one(t):
            for i in range(pairs):
                dst[pl.ds(pl.multiple_of(t * SLOT, 8) + 2 * i, 2), :] = src[t, i].astype(F32)

        loop(chips, one, unroll=4)

    def pack(src, dst):
        def one(t):
            for i in range(pairs):
                at = pl.ds(pl.multiple_of(t * SLOT, 8) + 2 * i, 2)
                dst[t, i] = src[at, :].astype(BF16)

        return one

    def pack_rows(src, dst):
        def one(t):
            for i in range(pairs):
                dst[t, i] = src[pl.ds(2 * i * chips + t, 2, stride=chips), :].astype(BF16)

        return one

    def eight(src, g, r, kq):
        return src[pl.ds(g * 8 * SLOT + r * parts + kq, 8, stride=SLOT), :]

    def gather_rows(src, dst):
        for r in range(rows):
            for g in range(0, groups, 2):
                at = r * chips + g * 8
                for kq in range(parts):
                    dst[at : at + 16, kq * LANES : (kq + 1) * LANES] = jnp.concatenate(
                        [eight(src, g, r, kq), eight(src, g + 1, r, kq)], axis=0
                    ).astype(BF16)

    eye = (
        lax.broadcasted_iota(jnp.int32, (width, width), 0)
        == lax.broadcasted_iota(jnp.int32, (width, width), 1)
    ).astype(BF16)

    for load in loads[:3]:
        load.wait()

    def front(r, kq):
        q = cols(kq, r)
        z = dot(eye, act_ref[q, :], NT)
        center = z - jnp.mean(z, axis=0, keepdims=True)
        scale = lax.rsqrt(jnp.mean(center * center, axis=0, keepdims=True) + EPS)
        zhat = center * scale
        low = zhat.astype(BF16)
        zhat_s[:, q] = zhat
        zscale_s[:, q] = scale
        norm_s[:, q] = low
        projected = dot(proj_ref[...], low, TN)
        keeper = mask_ref[r : r + 1, cols(kq)].astype(F32)
        values = projected[: 2 * hidden]
        sigma = jax.nn.sigmoid(projected[2 * hidden :])
        p1 = keeper * sigma
        factors = p1 * values
        p1_s[:, q] = p1
        p2_s[:, q] = factors * (1.0 - sigma)
        for ab in range(2):
            for g in range(tall):
                at = ab * hidden + g * 8
                (spread, spread2)[ab][
                    pl.ds(g * 8 * SLOT + r * parts + kq, 8, stride=SLOT), :
                ] = factors[at : at + 8]

    cells(front, unroll=3)
    loop(chips, pack(spread2, s1b), unroll=4)
    loop(chips, pack(spread, s1a), unroll=4)
    pl.semaphore_wait(barrier, chips + side - 1)
    exchange(s1b, r1b, 0)
    exchange(s1a, r1a, 1)

    for load in loads[3:]:
        load.wait()
    within, across = (
        jnp.sum(eye.astype(F32) * bias_ref[e : e + 1, :], axis=1, keepdims=True) for e in range(2)
    )
    def gating(r, kq):
        q = cols(kq, r)
        same = chain_ref[cols(kq)].reshape(1, LANES) == own_ref[me * rows + r]
        logits = dot(gate_ref[...], norm_s[:, q], TN)
        logits = logits + jnp.where(same, within, across)
        gate = jax.nn.sigmoid(logits)
        up = dot(eye, grad_ref[q, :], NT) * gate
        low = up.astype(BF16)
        do_s[:, q] = low
        e_s[:, q] = up * (1.0 - gate)
        dh_s[:, q] = dot(outw_ref[...], low, NN)

    cells(gating, unroll=3)

    arrive(r1b, 0)
    first = to_partner(r1b, r1p, 0)
    unpack(r1b, spread2)

    def place_right(src, which):
        for r in range(rows):
            for g in range(groups):
                for kq in range(parts):
                    wide[kq, pl.ds(g * 48 + 3 * which + r, 8, stride=6), :] = eight(src, g, r, kq)

    place_right(spread2, core)
    first.wait()
    unpack(r1p, spread2)
    place_right(spread2, 1 - core)
    arrive(r1a, 1)
    unpack(r1a, spread)
    gather_rows(spread, a_s)
    for kq in range(parts):
        b_s[:, kq * LANES : (kq + 1) * LANES] = wide[kq].astype(BF16)
    for kq in range(parts):
        product = dot(a_s[...], b_s[kq * LANES : (kq + 1) * LANES, :], NT)
        for r in range(rows):
            at = (r * parts + kq) * chips
            flat[at : at + chips, :] = product[r * chips : (r + 1) * chips]
    exchange(s2, r2, 2, pack_rows(flat, s2))

    arrive(r2, 2)
    unpack(r2, spread)

    def middle(r, kq):
        q = cols(kq, r)
        tri = jnp.concatenate(
            [eight(spread, g, r, kq) for g in range(tall)], axis=0
        )
        center = tri - jnp.mean(tri, axis=0, keepdims=True)
        scale = lax.rsqrt(jnp.mean(center * center, axis=0, keepdims=True) + EPS)
        hat = center * scale
        low = hat.astype(BF16)
        trilow_s[:, q] = low
        outputs = dot(outw_ref[...], low, TN)
        dl_s[:, q] = (outputs * e_s[:, q]).astype(BF16)
        d_hat = dh_s[:, q]
        m1 = jnp.mean(d_hat, axis=0, keepdims=True)
        m2 = jnp.mean(d_hat * hat, axis=0, keepdims=True)
        d_tri = scale * (d_hat - m1 - hat * m2)
        for g in range(tall):
            spread2[pl.ds(g * 8 * SLOT + r * parts + kq, 8, stride=SLOT), :] = d_tri[
                g * 8 : g * 8 + 8
            ]

    cells(middle, unroll=3)

    exchange(s3, r3, 3, pack(spread2, s3))

    share = 2 * side
    spot = col * 2 + core

    def put(w, value):
        n = w.shape[1]
        for m in range(share):
            w[m] = value[m * n : (m + 1) * n].astype(BF16)

    def line_peers(fn):
        for d in far:
            for e in range(2):
                if d or e:
                    fn((row * side + lax.rem(col + d, side)) * 2 + (1 - core if e else core))

    def send(src, dst, k, device):
        pltpu.make_async_remote_copy(
            src_ref=src,
            dst_ref=dst,
            send_sem=line_send.at[k],
            recv_sem=line_recv.at[k],
            device_id={"cells": device},
            device_id_type=MESH,
        ).start()

    def scatter_line(src, dst, k):
        line_peers(lambda p: send(src.at[lax.rem(p, share)], dst.at[spot], k, p))
        pltpu.make_async_copy(src.at[spot], dst.at[spot], line_recv.at[k]).start()

    def reduce_column(src, mid, dst, k):
        pltpu.make_async_copy(src, src, line_recv.at[k - 1]).wait()
        mid[...] = jnp.sum(src[...].astype(F32), axis=0)
        for d in far[:-1]:
            p = (lax.rem(row + d, side) * side + col) * 2 + core
            send(mid, dst.at[row], k, p)
        pltpu.make_async_copy(mid, dst.at[row], line_recv.at[k]).start()

    def gather_line(src, mid, dst, k):
        pltpu.make_async_copy(src, src, line_recv.at[k - 1]).wait()
        mid[...] = (jnp.sum(src[...], axis=0) * (1.0 / length)).astype(BF16)
        line_peers(lambda p: send(mid, dst.at[spot], k, p))
        pltpu.make_async_copy(mid, dst.at[spot], line_recv.at[k]).start()

    def drain(w, column, full, k):
        for e, (src, n) in enumerate(((w, share), (column, side), (full, share))):
            view = src.at[pl.ds(0, n - 1)]
            pltpu.make_async_copy(view, view, line_send.at[k + e]).wait()

    put(
        w1,
        jnp.concatenate(
            [
                dot(norm_s[...], dl_s[...], NT),
                dot(trilow_s[...], do_s[...], NT),
                jnp.zeros((width - hidden, width), F32),
            ],
            axis=0,
        ),
    )
    scatter_line(w1, line1, 0)

    def gate_part(r, kq):
        q = cols(kq, r)
        dn_s[:, q] = dot(gate_ref[...], dl_s[:, q], NN)

    cells(gate_part, unroll=3)

    arrive(r3, 3)
    unpack(r3, spread)
    gather_rows(spread, dt_s)
    second = []
    for kq in range(parts):
        wide[kq] = dot(dt_s[...], a_s[:, kq * LANES : (kq + 1) * LANES], TN)
        for r in range(rows):
            for g in range(groups):
                half_s[kq, r * chips + g * 8 : r * chips + g * 8 + 8, :] = wide[
                    kq, pl.ds(g * 48 + 3 * (1 - core) + r, 8, stride=6), :
                ]
        second.append(to_partner(half_s.at[kq], half_r.at[kq], 1 + kq))
    for kq in range(parts):
        product = dot(dt_s[...], b_s[:, kq * LANES : (kq + 1) * LANES], NN)
        for r in range(rows):
            at = (r * parts + kq) * chips
            flat[at : at + chips, :] = product[r * chips : (r + 1) * chips]
    exchange(s4a, r4a, 4, pack_rows(flat, s4a))
    for kq in range(parts):
        second[kq].wait()
        for r in range(rows):
            for g in range(groups):
                at = (r * parts + kq) * chips + g * 8
                flat[at : at + 8, :] = (
                    wide[kq, pl.ds(g * 48 + 3 * core + r, 8, stride=6), :]
                    + half_r[kq, r * chips + g * 8 : r * chips + g * 8 + 8, :]
                )
    exchange(s4b, r4b, 5, pack_rows(flat, s4b))
    reduce_column(line1, mid1a, column1, 1)

    def half_back(ab, src, k, w, line, base):
        arrive(src, k)
        unpack(src, spread)
        at = slice(ab * hidden, (ab + 1) * hidden)
        up = slice((2 + ab) * hidden, (3 + ab) * hidden)

        def factor_back(r, kq):
            q = cols(kq, r)
            d_factors = jnp.concatenate(
                [eight(spread, g, r, kq) for g in range(tall)], axis=0
            )
            dproj_s[at, q] = (d_factors * p1_s[at, q]).astype(BF16)
            dproj_s[up, q] = (d_factors * p2_s[at, q]).astype(BF16)

        cells(factor_back, unroll=3)
        put(
            w,
            dot(norm_s[...], jnp.concatenate([dproj_s[at, :], dproj_s[up, :]], axis=0), NT),
        )
        scatter_line(w, line, base)

    half_back(0, r4a, 4, w2, line2, 3)
    half_back(1, r4b, 5, w3, line3, 6)
    gather_line(column1, mid1b, full1, 2)

    def finish(r, kq):
        q = cols(kq, r)
        d_norm = dot(proj_ref[...], dproj_s[:, q], NN) + dn_s[:, q]
        zhat = zhat_s[:, q]
        m1 = jnp.mean(d_norm, axis=0, keepdims=True)
        m2 = jnp.mean(d_norm * zhat, axis=0, keepdims=True)
        grad = zscale_s[:, q] * (d_norm - m1 - zhat * m2)
        pair_out[q, :] = grad.T.astype(BF16)

    reduce_column(line2, mid2a, column2, 4)
    cells(finish, unroll=3)
    reduce_column(line3, mid3a, column3, 7)
    gather_line(column2, mid2b, full2, 5)

    def landed(full, k):
        pltpu.make_async_copy(full, full, line_recv.at[k]).wait()
        return full[...].astype(F32).reshape(full.shape[0] * full.shape[1], width)

    gather_line(column3, mid3b, full3, 8)
    sums = landed(full1, 2)
    gate_out[...] = sums[0:width]
    out_out[...] = sums[width : width + hidden]
    for k, src in enumerate((s1b, s1a, s2, s3, s4a, s4b)):
        sent(src, k)
    drain(w1, column1, full1, 0)
    drain(w2, column2, full2, 3)
    left, right = landed(full2, 5), landed(full3, 8)
    lower = lax.broadcasted_iota(jnp.int32, left.shape, 1) < hidden
    proj_out[:, 0:width] = jnp.where(lower, left, pltpu.roll(right, hidden, 1))
    proj_out[:, width : 2 * width] = jnp.where(lower, pltpu.roll(left, hidden, 1), right)
    drain(w3, column3, full3, 6)


def write(a_ref, b_ref, c_ref, d_ref, a_out, b_out, c_out, d_out, sem):
    copies = [
        pltpu.make_async_copy(src, dst, sem.at[k])
        for k, (src, dst) in enumerate(
            ((a_ref, a_out), (b_ref, b_out), (c_ref, c_out), (d_ref, d_out))
        )
    ]
    for copy in copies:
        copy.start()
    for copy in copies:
        copy.wait()


def local(
    pair_act, pair_mask, chain_ids, proj_weight, gate_weight, chain_bias, out_weight, out_grad
):
    devices = lax.axis_size("cells")
    chips = devices // 2
    rows, length, width = pair_act.shape
    hidden = out_weight.shape[0]
    count = rows * length
    parts = length // LANES
    side = math.isqrt(chips)
    share = 2 * side
    vm = pl.BlockSpec(memory_space=pltpu.VMEM)
    hbm = pl.BlockSpec(memory_space=pltpu.HBM)
    V = pltpu.VMEM
    pairs = (rows * parts + 1) // 2
    slots = (chips, pairs, 2, LANES)

    def reduction(block):
        return [
            V((share, block, width), BF16),
            V((share, block, width), BF16),
            V((block, width), F32),
            V((side, block, width), F32),
            V((block, width), BF16),
            V((share, block, width), BF16),
        ]

    shapes = (
        jax.ShapeDtypeStruct((count, width), BF16),
        jax.ShapeDtypeStruct((width, 4 * hidden), F32),
        jax.ShapeDtypeStruct((width, width), F32),
        jax.ShapeDtypeStruct((hidden, width), F32),
    )
    out = pl.pallas_call(
        kernel,
        out_shape=shapes,
        in_specs=8 * [hbm],
        out_specs=(vm, vm, vm, vm),
        scratch_shapes=[
            V((count, width), BF16),
            V((count, width), BF16),
            V((rows, length), jnp.int32),
            V((length,), jnp.int32),
            pltpu.SMEM((length,), jnp.int32),
            V((width, 4 * hidden), BF16),
            V((width, width), BF16),
            V((2, width), F32),
            V((hidden, width), BF16),
            pltpu.SemaphoreType.DMA((9,)),
            V((width, count), F32),
            V((1, count), F32),
            V((width, count), BF16),
            V((2 * hidden, count), F32),
            V((2 * hidden, count), F32),
            V((width, count), BF16),
            V((width, count), F32),
            V((hidden, count), F32),
            V((width, count), BF16),
            V((width, count), F32),
            V((hidden, count), BF16),
            V((4 * hidden, count), BF16),
            V((SLOT * chips, LANES), F32),
            V((parts, length, LANES), F32),
            V((2 * pairs * chips, LANES), F32),
            V((rows * chips, length), BF16),
            V((length, length), BF16),
            V((rows * chips, length), BF16),
            V((SLOT * chips, LANES), F32),
            *(13 * [V(slots, BF16)]),
            V((parts, rows * chips, LANES), F32),
            V((parts, rows * chips, LANES), F32),
            *reduction(2 * width // share),
            *reduction(width // share),
            *reduction(width // share),
            pltpu.SemaphoreType.DMA((6,)),
            pltpu.SemaphoreType.DMA((6,)),
            pltpu.SemaphoreType.DMA((1 + parts,)),
            pltpu.SemaphoreType.DMA((1 + parts,)),
            pltpu.SemaphoreType.DMA((9,)),
            pltpu.SemaphoreType.DMA((9,)),
        ],
        compiler_params=pltpu.CompilerParams(
            collective_id=0, has_side_effects=True, vmem_limit_bytes=20 * 1024 * 1024
        ),
    )(
        *(
            pltpu.with_memory_space_constraint(x, pltpu.HBM)
            for x in (
                pair_act.reshape(count, width),
                out_grad.reshape(count, width),
                pair_mask,
                chain_ids,
                proj_weight,
                gate_weight,
                chain_bias,
                out_weight,
            )
        )
    )
    out = pl.pallas_call(
        write,
        out_shape=shapes,
        in_specs=4 * [vm],
        out_specs=tuple(4 * [hbm]),
        scratch_shapes=[pltpu.SemaphoreType.DMA((4,))],
        compiler_params=pltpu.CompilerParams(vmem_limit_bytes=4 * 1024 * 1024),
    )(*out)
    return (out[0].reshape(rows, length, width), out[1], out[2], out[3])


def solution(mesh):
    placed = (
        P(("groups", "cells"), None, None),
        P(("groups", "cells"), None),
        P("groups"),
        P(),
        P(),
        P(),
        P(),
        P(("groups", "cells"), None, None),
    )
    return jax.shard_map(
        local,
        mesh=mesh,
        in_specs=placed,
        out_specs=(
            P(("groups", "cells"), None, None),
            P("groups", None),
            P("groups", None),
            P("groups", None),
        ),
        check_vma=False,
    )
```

```python
import math

import jax
import jax.numpy as jnp
from jax import lax
from jax.experimental import pallas as pl
from jax.experimental.pallas import tpu as pltpu
from jax.sharding import PartitionSpec as P

EPS = 1e-05
MESH = pl.DeviceIdType.MESH
F32 = jnp.float32
BF16 = jnp.bfloat16
LANES = 128
SLOT = 24
NT = (((1,), (1,)), ((), ()))
TN = (((0,), (0,)), ((), ()))
NN = (((1,), (0,)), ((), ()))


def dot(a, b, dims):
    return lax.dot_general(a, b, dims, preferred_element_type=F32)


def loop(n, body, unroll=1):
    def step(i, carry):
        body(i)
        return carry

    lax.fori_loop(0, n, step, 0, unroll=unroll)


def kernel(
    act_hbm,
    grad_hbm,
    mask_hbm,
    chain_hbm,
    proj_hbm,
    gate_hbm,
    bias_hbm,
    outw_hbm,
    pair_out,
    proj_out,
    gate_out,
    out_out,
    act_ref,
    grad_ref,
    mask_ref,
    chain_ref,
    own_ref,
    proj_ref,
    gate_ref,
    bias_ref,
    outw_ref,
    in_sem,
    zhat_s,
    zscale_s,
    norm_s,
    p1_s,
    p2_s,
    do_s,
    e_s,
    dh_s,
    dl_s,
    dn_s,
    trilow_s,
    dproj_s,
    spread,
    wide,
    flat,
    a_s,
    b_s,
    dt_s,
    spread2,
    s1a,
    s1b,
    s2,
    s3,
    s4a,
    s4b,
    r1a,
    r1b,
    r1p,
    r2,
    r3,
    r4a,
    r4b,
    half_s,
    half_r,
    w1,
    line1,
    mid1a,
    column1,
    mid1b,
    full1,
    few,
    projt_s,
    col_recv,
    w2,
    line2,
    mid2a,
    column2,
    mid2b,
    full2,
    w3,
    line3,
    mid3a,
    column3,
    mid3b,
    full3,
    send_sem,
    recv_sem,
    pair_send,
    pair_recv,
    line_send,
    line_recv,
):
    loads = [
        pltpu.make_async_copy(src, dst, in_sem.at[k])
        for k, (src, dst) in enumerate(
            (
                (act_hbm, act_ref),
                (proj_hbm, proj_ref),
                (mask_hbm, mask_ref),
                (grad_hbm, grad_ref),
                (gate_hbm, gate_ref),
                (outw_hbm, outw_ref),
                (bias_hbm, bias_ref),
                (chain_hbm, chain_ref),
                (chain_hbm, own_ref),
            )
        )
    ]
    for load in loads:
        load.start()
    me = lax.axis_index("cells")
    devices = lax.axis_size("cells")
    chips = devices // 2
    side = math.isqrt(chips)
    chip = me // 2
    core = lax.rem(me, 2)
    row, col = chip // side, lax.rem(chip, side)
    far = sorted(range(side), key=lambda d: -min(d, side - d))
    partner = me + 1 - 2 * core
    rows, length = mask_ref.shape
    width = act_ref.shape[1]
    hidden = outw_ref.shape[0]
    parts = length // LANES
    tall = hidden // 8
    groups = chips // 8
    pairs = (rows * parts + 1) // 2

    barrier = pltpu.get_barrier_semaphore()

    def base_of(i):
        step = side // 2 + ((i + 1) // 2) * (1 - 2 * lax.rem(i, 2))
        return lax.rem(row + step, side) * side

    def each_chip(fn, prepare=None):
        def line(i):
            base, later = base_of(i), base_of(i + 1)
            for k, d in enumerate(far):
                if prepare is not None:
                    prepare(later + k)
                fn(base + lax.rem(col + d, side))

        if prepare is not None:
            for k in range(side):
                prepare(base_of(jnp.int32(0)) + k)
        loop(side - 1, line)
        for d in far[:-1]:
            fn(row * side + lax.rem(col + d, side))

    def greet(peer):
        pl.semaphore_signal(barrier, inc=1, device_id={"cells": peer}, device_id_type=MESH)

    each_chip(lambda t: greet(t * 2 + core))
    for d in far[:-1]:
        greet((row * side + lax.rem(col + d, side)) * 2 + 1 - core)
    greet(partner)

    def exchange(src, dst, k, prepare=None, recv=None):
        recv = recv_sem.at[k] if recv is None else recv

        def one(t):
            pltpu.make_async_remote_copy(
                src_ref=src.at[t],
                dst_ref=dst.at[chip],
                send_sem=send_sem.at[k],
                recv_sem=recv,
                device_id={"cells": t * 2 + core},
                device_id_type=MESH,
            ).start()

        each_chip(one, prepare)
        pltpu.make_async_copy(src.at[chip], dst.at[chip], recv).start()

    def arrive(dst, k):
        pltpu.make_async_copy(dst, dst, recv_sem.at[k]).wait()

    def sent(src, k):
        view = src.at[pl.ds(0, chips - 1)]
        pltpu.make_async_copy(view, view, send_sem.at[k]).wait()

    def to_partner(src, dst, k):
        copy = pltpu.make_async_remote_copy(
            src_ref=src,
            dst_ref=dst,
            send_sem=pair_send.at[k],
            recv_sem=pair_recv.at[k],
            device_id={"cells": partner},
            device_id_type=MESH,
        )
        copy.start()
        return copy

    def cols(kq, r=0):
        return pl.ds(pl.multiple_of((r * parts + kq) * LANES, LANES), LANES)

    def cells(body, unroll=1):
        for r in range(rows):
            loop(parts, lambda kq, r=r: body(r, kq), unroll)

    lead = side * SLOT + 8

    def slot(t):
        return pl.multiple_of(t * SLOT + t // side * 8, 8)

    def unpack(src, dst):
        def one(t):
            for i in range(pairs):
                dst[pl.ds(slot(t) + 2 * i, 2), :] = src[t, i].astype(F32)

        loop(chips, one, unroll=4)

    def pack(src, dst):
        def one(t):
            for i in range(pairs):
                at = pl.ds(slot(t) + 2 * i, 2)
                dst[t, i] = src[at, :].astype(BF16)

        return one

    def pack_rows(src, dst):
        def one(t):
            for i in range(pairs):
                dst[t, i] = src[pl.ds(2 * i * chips + t, 2, stride=chips), :].astype(BF16)

        return one

    def eight(src, g, r, kq):
        return src[pl.ds(g * lead + r * parts + kq, 8, stride=SLOT), :]

    def channels(g, r, kq):
        return pl.ds(g * SLOT + r * parts + kq, 8, stride=lead)

    def gather_rows(src, dst):
        for r in range(rows):
            for g in range(0, groups, 2):
                at = r * chips + g * 8
                for kq in range(parts):
                    dst[at : at + 16, kq * LANES : (kq + 1) * LANES] = jnp.concatenate(
                        [eight(src, g, r, kq), eight(src, g + 1, r, kq)], axis=0
                    ).astype(BF16)

    eye = (
        lax.broadcasted_iota(jnp.int32, (width, width), 0)
        == lax.broadcasted_iota(jnp.int32, (width, width), 1)
    ).astype(BF16)

    for load in loads[:3]:
        load.wait()

    def front(r, kq):
        q = cols(kq, r)
        z = dot(eye, act_ref[q, :], NT)
        center = z - jnp.mean(z, axis=0, keepdims=True)
        scale = lax.rsqrt(jnp.mean(center * center, axis=0, keepdims=True) + EPS)
        zhat = center * scale
        low = zhat.astype(BF16)
        zhat_s[:, q] = zhat
        zscale_s[:, q] = scale
        norm_s[:, q] = low
        projected = dot(proj_ref[...], low, TN)
        keeper = mask_ref[r : r + 1, cols(kq)].astype(F32)
        values = projected[: 2 * hidden]
        sigma = jax.nn.sigmoid(projected[2 * hidden :])
        p1 = keeper * sigma
        factors = p1 * values
        p1_s[:, q] = p1
        p2_s[:, q] = factors * (1.0 - sigma)
        for ab in range(2):
            for g in range(tall):
                at = ab * hidden + g * 8
                (spread, spread2)[ab][
                    channels(g, r, kq), :
                ] = factors[at : at + 8]

    cells(front, unroll=3)
    loop(chips, pack(spread2, s1b), unroll=4)
    loop(chips, pack(spread, s1a), unroll=4)
    pl.semaphore_wait(barrier, chips + side - 1)
    exchange(s1b, r1b, 0)
    exchange(s1a, r1a, 1)

    for load in loads[3:]:
        load.wait()
    within, across = (
        jnp.sum(eye.astype(F32) * bias_ref[e : e + 1, :], axis=1, keepdims=True) for e in range(2)
    )
    def gating(r, kq):
        q = cols(kq, r)
        same = chain_ref[cols(kq)].reshape(1, LANES) == own_ref[me * rows + r]
        logits = dot(gate_ref[...], norm_s[:, q], TN)
        logits = logits + jnp.where(same, within, across)
        gate = jax.nn.sigmoid(logits)
        up = dot(eye, grad_ref[q, :], NT) * gate
        low = up.astype(BF16)
        do_s[:, q] = low
        e_s[:, q] = up * (1.0 - gate)
        dh_s[:, q] = dot(outw_ref[...], low, NN)

    cells(gating, unroll=3)
    flipped = proj_ref[...].astype(F32).T
    for ab in range(2):
        for x in range(side):
            both = [
                flipped[(2 * e + ab) * hidden + x * 8 : (2 * e + ab) * hidden + x * 8 + 8]
                for e in range(2)
            ]
            at = 2 * (ab * hidden + x * 8)
            projt_s[at : at + 16, :] = jnp.concatenate(both, axis=0).astype(BF16)

    arrive(r1b, 0)
    first = to_partner(r1b, r1p, 0)
    unpack(r1b, spread2)

    def place_right(src, which):
        for r in range(rows):
            for g in range(groups):
                for kq in range(parts):
                    wide[kq, pl.ds(g * 48 + 3 * which + r, 8, stride=6), :] = eight(src, g, r, kq)

    place_right(spread2, core)
    first.wait()
    unpack(r1p, spread2)
    place_right(spread2, 1 - core)
    arrive(r1a, 1)
    unpack(r1a, spread)
    gather_rows(spread, a_s)
    for kq in range(parts):
        b_s[:, kq * LANES : (kq + 1) * LANES] = wide[kq].astype(BF16)
    for kq in range(parts):
        product = dot(a_s[...], b_s[kq * LANES : (kq + 1) * LANES, :], NT)
        for r in range(rows):
            at = (r * parts + kq) * chips
            flat[at : at + chips, :] = product[r * chips : (r + 1) * chips]
    exchange(s2, r2, 2, pack_rows(flat, s2))

    arrive(r2, 2)
    unpack(r2, spread)

    def middle(r, kq):
        q = cols(kq, r)
        tri = jnp.concatenate(
            [spread[channels(g, r, kq), :] for g in range(tall)], axis=0
        )
        center = tri - jnp.mean(tri, axis=0, keepdims=True)
        scale = lax.rsqrt(jnp.mean(center * center, axis=0, keepdims=True) + EPS)
        hat = center * scale
        low = hat.astype(BF16)
        trilow_s[:, q] = low
        outputs = dot(outw_ref[...], low, TN)
        dl_s[:, q] = (outputs * e_s[:, q]).astype(BF16)
        d_hat = dh_s[:, q]
        m1 = jnp.mean(d_hat, axis=0, keepdims=True)
        m2 = jnp.mean(d_hat * hat, axis=0, keepdims=True)
        d_tri = scale * (d_hat - m1 - hat * m2)
        for g in range(tall):
            spread2[channels(g, r, kq), :] = d_tri[
                g * 8 : g * 8 + 8
            ]

    cells(middle, unroll=3)

    exchange(s3, r3, 3, pack(spread2, s3))

    share = 2 * side
    spot = col * 2 + core

    def put(w, value):
        n = w.shape[1]
        for m in range(share):
            w[m] = value[m * n : (m + 1) * n].astype(BF16)

    def line_peers(fn):
        for d in far:
            for e in range(2):
                if d or e:
                    fn((row * side + lax.rem(col + d, side)) * 2 + (1 - core if e else core))

    def send(src, dst, k, device):
        pltpu.make_async_remote_copy(
            src_ref=src,
            dst_ref=dst,
            send_sem=line_send.at[k],
            recv_sem=line_recv.at[k],
            device_id={"cells": device},
            device_id_type=MESH,
        ).start()

    def scatter_line(src, dst, k):
        line_peers(lambda p: send(src.at[lax.rem(p, share)], dst.at[spot], k, p))
        pltpu.make_async_copy(src.at[spot], dst.at[spot], line_recv.at[k]).start()

    def reduce_column(src, mid, dst, k):
        pltpu.make_async_copy(src, src, line_recv.at[k - 1]).wait()
        mid[...] = jnp.sum(src[...].astype(F32), axis=0)
        for d in far[:-1]:
            p = (lax.rem(row + d, side) * side + col) * 2 + core
            send(mid, dst.at[row], k, p)
        pltpu.make_async_copy(mid, dst.at[row], line_recv.at[k]).start()

    def gather_line(src, mid, dst, k):
        pltpu.make_async_copy(src, src, line_recv.at[k - 1]).wait()
        mid[...] = (jnp.sum(src[...], axis=0) * (1.0 / length)).astype(BF16)
        line_peers(lambda p: send(mid, dst.at[spot], k, p))
        pltpu.make_async_copy(mid, dst.at[spot], line_recv.at[k]).start()

    def drain(w, column, full, k):
        for e, (src, n) in enumerate(((full, share), (column, side), (full, share))):
            view = src.at[pl.ds(0, n - 1)]
            pltpu.make_async_copy(view, view, line_send.at[k + e]).wait()

    put(
        w1,
        jnp.concatenate(
            [
                dot(norm_s[...], dl_s[...], NT),
                dot(trilow_s[...], do_s[...], NT),
                jnp.zeros((width - hidden, width), F32),
            ],
            axis=0,
        ),
    )
    scatter_line(w1, line1, 0)

    def gate_part(r, kq):
        q = cols(kq, r)
        dn_s[:, q] = dot(gate_ref[...], dl_s[:, q], NN)

    cells(gate_part, unroll=3)

    arrive(r3, 3)
    unpack(r3, spread)
    gather_rows(spread, dt_s)
    second = []
    for kq in range(parts):
        wide[kq] = dot(dt_s[...], a_s[:, kq * LANES : (kq + 1) * LANES], TN)
        for r in range(rows):
            for g in range(groups):
                half_s[kq, r * chips + g * 8 : r * chips + g * 8 + 8, :] = wide[
                    kq, pl.ds(g * 48 + 3 * (1 - core) + r, 8, stride=6), :
                ]
        second.append(to_partner(half_s.at[kq], half_r.at[kq], 1 + kq))
    for kq in range(parts):
        product = dot(dt_s[...], b_s[:, kq * LANES : (kq + 1) * LANES], NN)
        for r in range(rows):
            at = (r * parts + kq) * chips
            flat[at : at + chips, :] = product[r * chips : (r + 1) * chips]
    exchange(s4a, r4a, 4, pack_rows(flat, s4a), col_recv.at[0, col])
    for kq in range(parts):
        second[kq].wait()
        for r in range(rows):
            for g in range(groups):
                at = (r * parts + kq) * chips + g * 8
                flat[at : at + 8, :] = (
                    wide[kq, pl.ds(g * 48 + 3 * core + r, 8, stride=6), :]
                    + half_r[kq, r * chips + g * 8 : r * chips + g * 8 + 8, :]
                )
    exchange(s4b, r4b, 5, pack_rows(flat, s4b), col_recv.at[1, col])
    reduce_column(line1, mid1a, column1, 1)

    def half_back(ab, src, w, line, k):
        for d in reversed(far):
            x = lax.rem(col + d, side)
            view = src.at[pl.ds(0, side)]
            pltpu.make_async_copy(view, view, col_recv.at[ab, x]).wait()
            for y in range(side):
                for i in range(pairs):
                    few[y * SLOT + 2 * i : y * SLOT + 2 * i + 2, :] = src[
                        y * side + x, i
                    ].astype(F32)
            at = pl.ds(pl.multiple_of(ab * hidden + x * 8, 8), 8)
            to = pl.ds(pl.multiple_of(2 * (ab * hidden + x * 8), 16), 16)
            for r in range(rows):
                for kq in range(parts):
                    q = slice((r * parts + kq) * LANES, (r * parts + kq + 1) * LANES)
                    d_factors = few[pl.ds(r * parts + kq, 8, stride=SLOT), :]
                    both = [d_factors * p1_s[at, q], d_factors * p2_s[at, q]]
                    dproj_s[to, q] = jnp.concatenate(both, axis=0).astype(BF16)
            term = dot(dproj_s[to, :], norm_s[...], NT)
            across_line = (row * side + lax.rem(x + side // 2, side)) * 2
            for e in range(2):
                w[x, e] = term[8 * e : 8 * e + 8].astype(BF16)
            for e in range(2):
                half = 1 - core if e else core
                if e or d != side // 2:
                    send(w.at[x, half], line.at[spot], k, across_line + half)
                else:
                    pltpu.make_async_copy(w.at[x, half], line.at[spot], line_recv.at[k]).start()

    half_back(0, r4a, w2, line2, 3)
    half_back(1, r4b, w3, line3, 6)
    gather_line(column1, mid1b, full1, 2)

    def finish(r, kq):
        q = cols(kq, r)
        d_norm = dot(projt_s[...], dproj_s[:, q], TN) + dn_s[:, q]
        zhat = zhat_s[:, q]
        m1 = jnp.mean(d_norm, axis=0, keepdims=True)
        m2 = jnp.mean(d_norm * zhat, axis=0, keepdims=True)
        grad = zscale_s[:, q] * (d_norm - m1 - zhat * m2)
        pair_out[q, :] = grad.T.astype(BF16)

    reduce_column(line2, mid2a, column2, 4)
    cells(finish, unroll=3)
    reduce_column(line3, mid3a, column3, 7)
    gather_line(column2, mid2b, full2, 5)

    def landed(full, k):
        pltpu.make_async_copy(full, full, line_recv.at[k]).wait()
        return full[...].astype(F32).reshape(full.shape[0] * full.shape[1], width)

    gather_line(column3, mid3b, full3, 8)
    sums = landed(full1, 2)
    gate_out[...] = sums[0:width]
    out_out[...] = sums[width : width + hidden]
    for k, src in enumerate((s1b, s1a, s2, s3, s4a, s4b)):
        sent(src, k)
    drain(w1, column1, full1, 0)
    drain(w2, column2, full2, 3)
    pltpu.make_async_copy(full2, full2, line_recv.at[5]).wait()
    pltpu.make_async_copy(full3, full3, line_recv.at[8]).wait()
    for e in range(2):
        turned = [
            full[2 * ((x + side // 2) % side) + e].astype(F32)
            for full in (full2, full3)
            for x in range(side)
        ]
        proj_out[:, e * width : (e + 1) * width] = jnp.concatenate(turned, axis=0).T
    drain(w3, column3, full3, 6)


def write(a_ref, b_ref, c_ref, d_ref, a_out, b_out, c_out, d_out, sem):
    copies = [
        pltpu.make_async_copy(src, dst, sem.at[k])
        for k, (src, dst) in enumerate(
            ((a_ref, a_out), (b_ref, b_out), (c_ref, c_out), (d_ref, d_out))
        )
    ]
    for copy in copies:
        copy.start()
    for copy in copies:
        copy.wait()


def local(
    pair_act, pair_mask, chain_ids, proj_weight, gate_weight, chain_bias, out_weight, out_grad
):
    devices = lax.axis_size("cells")
    chips = devices // 2
    rows, length, width = pair_act.shape
    hidden = out_weight.shape[0]
    count = rows * length
    parts = length // LANES
    side = math.isqrt(chips)
    assert side == 8 and hidden == chips
    share = 2 * side
    vm = pl.BlockSpec(memory_space=pltpu.VMEM)
    hbm = pl.BlockSpec(memory_space=pltpu.HBM)
    V = pltpu.VMEM
    pairs = (rows * parts + 1) // 2
    slots = (chips, pairs, 2, LANES)

    def reduction(block):
        return [
            V((share, block, width), BF16),
            V((share, block, width), BF16),
            V((block, width), F32),
            V((side, block, width), F32),
            V((block, width), BF16),
            V((share, block, width), BF16),
        ]

    def by_column(block):
        return [V((side, 2, block, width), BF16), *reduction(block)[1:]]

    shapes = (
        jax.ShapeDtypeStruct((count, width), BF16),
        jax.ShapeDtypeStruct((width, 4 * hidden), F32),
        jax.ShapeDtypeStruct((width, width), F32),
        jax.ShapeDtypeStruct((hidden, width), F32),
    )
    out = pl.pallas_call(
        kernel,
        out_shape=shapes,
        in_specs=8 * [hbm],
        out_specs=(vm, vm, vm, vm),
        scratch_shapes=[
            V((count, width), BF16),
            V((count, width), BF16),
            V((rows, length), jnp.int32),
            V((length,), jnp.int32),
            pltpu.SMEM((length,), jnp.int32),
            V((width, 4 * hidden), BF16),
            V((width, width), BF16),
            V((2, width), F32),
            V((hidden, width), BF16),
            pltpu.SemaphoreType.DMA((9,)),
            V((width, count), F32),
            V((1, count), F32),
            V((width, count), BF16),
            V((2 * hidden, count), F32),
            V((2 * hidden, count), F32),
            V((width, count), BF16),
            V((width, count), F32),
            V((hidden, count), F32),
            V((width, count), BF16),
            V((width, count), F32),
            V((hidden, count), BF16),
            V((4 * hidden, count), BF16),
            V((SLOT * chips + 8 * side, LANES), F32),
            V((parts, length, LANES), F32),
            V((2 * pairs * chips, LANES), F32),
            V((rows * chips, length), BF16),
            V((length, length), BF16),
            V((rows * chips, length), BF16),
            V((SLOT * chips + 8 * side, LANES), F32),
            *(13 * [V(slots, BF16)]),
            V((parts, rows * chips, LANES), F32),
            V((parts, rows * chips, LANES), F32),
            *reduction(2 * width // share),
            V((8 * SLOT, LANES), F32),
            V((4 * hidden, width), BF16),
            pltpu.SemaphoreType.DMA((2, side)),
            *by_column(width // share),
            *by_column(width // share),
            pltpu.SemaphoreType.DMA((6,)),
            pltpu.SemaphoreType.DMA((6,)),
            pltpu.SemaphoreType.DMA((1 + parts,)),
            pltpu.SemaphoreType.DMA((1 + parts,)),
            pltpu.SemaphoreType.DMA((9,)),
            pltpu.SemaphoreType.DMA((9,)),
        ],
        compiler_params=pltpu.CompilerParams(
            collective_id=0, has_side_effects=True, vmem_limit_bytes=20 * 1024 * 1024
        ),
    )(
        *(
            pltpu.with_memory_space_constraint(x, pltpu.HBM)
            for x in (
                pair_act.reshape(count, width),
                out_grad.reshape(count, width),
                pair_mask,
                chain_ids,
                proj_weight,
                gate_weight,
                chain_bias,
                out_weight,
            )
        )
    )
    out = pl.pallas_call(
        write,
        out_shape=shapes,
        in_specs=4 * [vm],
        out_specs=tuple(4 * [hbm]),
        scratch_shapes=[pltpu.SemaphoreType.DMA((4,))],
        compiler_params=pltpu.CompilerParams(vmem_limit_bytes=4 * 1024 * 1024),
    )(*out)
    return (out[0].reshape(rows, length, width), out[1], out[2], out[3])


def solution(mesh):
    placed = (
        P(("groups", "cells"), None, None),
        P(("groups", "cells"), None),
        P("groups"),
        P(),
        P(),
        P(),
        P(),
        P(("groups", "cells"), None, None),
    )
    return jax.shard_map(
        local,
        mesh=mesh,
        in_specs=placed,
        out_specs=(
            P(("groups", "cells"), None, None),
            P("groups", None),
            P("groups", None),
            P("groups", None),
        ),
        check_vma=False,
    )
```

```python
import math

import jax
import jax.numpy as jnp
from jax import lax
from jax.experimental import pallas as pl
from jax.experimental.pallas import tpu as pltpu
from jax.sharding import PartitionSpec as P

EPS = 1e-05
MESH = pl.DeviceIdType.MESH
F32 = jnp.float32
BF16 = jnp.bfloat16
LANES = 128
SLOT = 24
NT = (((1,), (1,)), ((), ()))
TN = (((0,), (0,)), ((), ()))
NN = (((1,), (0,)), ((), ()))


def dot(a, b, dims):
    return lax.dot_general(a, b, dims, preferred_element_type=F32)


def loop(n, body, unroll=1):
    def step(i, carry):
        body(i)
        return carry

    lax.fori_loop(0, n, step, 0, unroll=unroll)


def kernel(
    act_hbm,
    grad_hbm,
    mask_hbm,
    chain_hbm,
    proj_hbm,
    gate_hbm,
    bias_hbm,
    outw_hbm,
    pair_out,
    proj_out,
    gate_out,
    out_out,
    act_ref,
    grad_ref,
    mask_ref,
    chain_ref,
    own_ref,
    proj_ref,
    gate_ref,
    bias_ref,
    outw_ref,
    in_sem,
    zhat_s,
    zscale_s,
    norm_s,
    p1_s,
    p2_s,
    do_s,
    e_s,
    dh_s,
    dl_s,
    dn_s,
    trilow_s,
    dproj_s,
    spread,
    wide,
    flat,
    a_s,
    b_s,
    dt_s,
    spread2,
    s1a,
    s1b,
    s2,
    s3,
    s4a,
    s4b,
    r1a,
    r1b,
    r1p,
    r2,
    r3,
    r4a,
    r4b,
    half_s,
    half_r,
    w1,
    line1,
    mid1a,
    column1,
    mid1b,
    full1,
    few,
    projt_s,
    col_recv,
    w2,
    line2,
    mid2a,
    column2,
    mid2b,
    full2,
    w3,
    line3,
    mid3a,
    column3,
    mid3b,
    full3,
    send_sem,
    recv_sem,
    pair_send,
    pair_recv,
    line_send,
    line_recv,
):
    loads = [
        pltpu.make_async_copy(src, dst, in_sem.at[k])
        for k, (src, dst) in enumerate(
            (
                (act_hbm, act_ref),
                (proj_hbm, proj_ref),
                (mask_hbm, mask_ref),
                (grad_hbm, grad_ref),
                (gate_hbm, gate_ref),
                (outw_hbm, outw_ref),
                (bias_hbm, bias_ref),
                (chain_hbm, chain_ref),
                (chain_hbm, own_ref),
            )
        )
    ]
    for load in loads:
        load.start()
    me = lax.axis_index("cells")
    devices = lax.axis_size("cells")
    chips = devices // 2
    side = math.isqrt(chips)
    chip = me // 2
    core = lax.rem(me, 2)
    row, col = chip // side, lax.rem(chip, side)
    far = sorted(range(side), key=lambda d: -min(d, side - d))
    partner = me + 1 - 2 * core
    rows, length = mask_ref.shape
    width = act_ref.shape[1]
    hidden = outw_ref.shape[0]
    parts = length // LANES
    tall = hidden // 8
    groups = chips // 8
    pairs = (rows * parts + 1) // 2

    barrier = pltpu.get_barrier_semaphore()

    def line_of(i):
        step = side // 2 + ((i + 1) // 2) * (1 - 2 * lax.rem(i, 2))
        return lax.rem(row + step, side)

    def each_chip(fn, prepare=None):
        def line(i):
            now, later = line_of(i), line_of(i + 1)
            for x, d in enumerate(far):
                if prepare is not None:
                    prepare(later, x)
                fn(now * side + lax.rem(col + d, side))

        if prepare is not None:
            for x in range(side):
                prepare(line_of(jnp.int32(0)), x)
        loop(side - 1, line)
        for d in far[:-1]:
            fn(row * side + lax.rem(col + d, side))

    def greet(peer):
        pl.semaphore_signal(barrier, inc=1, device_id={"cells": peer}, device_id_type=MESH)

    each_chip(lambda t: greet(t * 2 + core))
    for d in far[:-1]:
        greet((row * side + lax.rem(col + d, side)) * 2 + 1 - core)
    greet(partner)

    def exchange(src, dst, k, prepare=None, recv=None):
        recv = recv_sem.at[k, row] if recv is None else recv

        def one(t):
            pltpu.make_async_remote_copy(
                src_ref=src.at[t],
                dst_ref=dst.at[chip],
                send_sem=send_sem.at[k],
                recv_sem=recv,
                device_id={"cells": t * 2 + core},
                device_id_type=MESH,
            ).start()

        each_chip(one, prepare)
        pltpu.make_async_copy(src.at[chip], dst.at[chip], recv).start()

    def sent(src, k):
        view = src.at[pl.ds(0, chips - 1)]
        pltpu.make_async_copy(view, view, send_sem.at[k]).wait()

    def to_partner(src, dst, k):
        copy = pltpu.make_async_remote_copy(
            src_ref=src,
            dst_ref=dst,
            send_sem=pair_send.at[k],
            recv_sem=pair_recv.at[k],
            device_id={"cells": partner},
            device_id_type=MESH,
        )
        copy.start()
        return copy

    def cols(kq, r=0):
        return pl.ds(pl.multiple_of((r * parts + kq) * LANES, LANES), LANES)

    def cells(body, unroll=1):
        for r in range(rows):
            loop(parts, lambda kq, r=r: body(r, kq), unroll)

    lead = side * SLOT + 8

    def slot(y, x):
        return pl.multiple_of(y * lead + x * SLOT, 8)

    def unpack(src, dst, k=None, then=None):
        def one(i):
            y = line_of(side - 1 - i)
            line = pl.ds(y * side, side)
            if k is not None:
                pltpu.make_async_copy(src.at[line], src.at[line], recv_sem.at[k, y]).wait()
            if then is not None:
                then(line)
            for x in range(side):
                for i in range(src.shape[1]):
                    dst[pl.ds(slot(y, x) + 2 * i, 2), :] = src[y * side + x, i].astype(F32)

        loop(side, one)

    def pack(src, dst):
        def one(y, x):
            for i in range(dst.shape[1]):
                at = pl.ds(slot(y, x) + 2 * i, 2)
                dst[y * side + x, i] = src[at, :].astype(BF16)

        return one

    def pack_rows(src, dst):
        def one(y, x):
            t = y * side + x
            for i in range(pairs):
                dst[t, i] = src[pl.ds(2 * i * chips + t, 2, stride=chips), :].astype(BF16)

        return one

    def eight(src, g, r, kq):
        return src[pl.ds(g * lead + r * parts + kq, 8, stride=SLOT), :]

    def channels(g, r, kq):
        return pl.ds(g * SLOT + r * parts + kq, 8, stride=lead)

    def gather_row(src, dst, r, kq, start):
        for g in range(0, groups, 2):
            at = r * chips + g * 8
            dst[at : at + 16, kq * LANES : (kq + 1) * LANES] = jnp.concatenate(
                [eight(src, g, 0, start), eight(src, g + 1, 0, start)], axis=0
            ).astype(BF16)

    def gather_rows(src, dst, n):
        for k in range(n):
            gather_row(src, dst, k // parts, k % parts, k)

    eye = (
        lax.broadcasted_iota(jnp.int32, (width, width), 0)
        == lax.broadcasted_iota(jnp.int32, (width, width), 1)
    ).astype(BF16)

    for load in loads[:3]:
        load.wait()

    def front(r, kq):
        q = cols(kq, r)
        z = dot(eye, act_ref[q, :], NT)
        center = z - jnp.mean(z, axis=0, keepdims=True)
        scale = lax.rsqrt(jnp.mean(center * center, axis=0, keepdims=True) + EPS)
        zhat = center * scale
        low = zhat.astype(BF16)
        zhat_s[:, q] = zhat
        zscale_s[:, q] = scale
        norm_s[:, q] = low
        projected = dot(proj_ref[...], low, TN)
        keeper = mask_ref[r : r + 1, cols(kq)].astype(F32)
        values = projected[: 2 * hidden]
        sigma = jax.nn.sigmoid(projected[2 * hidden :])
        p1 = keeper * sigma
        factors = p1 * values
        p1_s[:, q] = p1
        p2_s[:, q] = factors * (1.0 - sigma)
        for ab in range(2):
            for g in range(tall):
                at = ab * hidden + g * 8
                (spread, spread2)[ab][
                    channels(g, r, kq), :
                ] = factors[at : at + 8]
                if ab == 0 and r == rows - 1:
                    spread2[channels(g, rows, 0), :] = factors[at : at + 8]

    cells(front, unroll=3)
    def pack_all(y):
        for src, dst in ((spread2, s1b), (spread, s1a)):
            for x in range(side):
                pack(src, dst)(y, x)

    loop(side, pack_all)
    pl.semaphore_wait(barrier, chips + side - 1)
    exchange(s1b, r1b, 0)
    exchange(s1a, r1a, 1)

    for load in loads[3:]:
        load.wait()
    within, across = (
        jnp.sum(eye.astype(F32) * bias_ref[e : e + 1, :], axis=1, keepdims=True) for e in range(2)
    )
    def gating(r, kq):
        q = cols(kq, r)
        same = chain_ref[cols(kq)].reshape(1, LANES) == own_ref[me * rows + r]
        logits = dot(gate_ref[...], norm_s[:, q], TN)
        logits = logits + jnp.where(same, within, across)
        gate = jax.nn.sigmoid(logits)
        up = dot(eye, grad_ref[q, :], NT) * gate
        low = up.astype(BF16)
        do_s[:, q] = low
        e_s[:, q] = up * (1.0 - gate)
        dh_s[:, q] = dot(outw_ref[...], low, NN)

    cells(gating, unroll=3)
    flipped = proj_ref[...].astype(F32).T
    for ab in range(2):
        for x in range(side):
            both = [
                flipped[(2 * e + ab) * hidden + x * 8 : (2 * e + ab) * hidden + x * 8 + 8]
                for e in range(2)
            ]
            at = 2 * (ab * hidden + x * 8)
            projt_s[at : at + 16, :] = jnp.concatenate(both, axis=0).astype(BF16)

    unpack(r1b, spread2, 0, lambda at: to_partner(r1b.at[at], r1p.at[at], 0))

    def place_right(src, which):
        for r in range(rows):
            for g in range(groups):
                for kq in range(parts):
                    wide[kq, pl.ds(g * 48 + 3 * which + r, 8, stride=6), :] = eight(src, g, r, kq)

    place_right(spread2, core)
    gather_row(spread2, a_s, rows - 1, parts - 1, rows * parts)
    pltpu.make_async_copy(r1p, r1p, pair_recv.at[0]).wait()
    unpack(r1p, spread2)
    place_right(spread2, 1 - core)
    unpack(r1a, spread, 1)
    gather_rows(spread, a_s, rows * parts - 1)
    for kq in range(parts):
        b_s[:, kq * LANES : (kq + 1) * LANES] = wide[kq].astype(BF16)
    for kq in range(parts):
        product = dot(a_s[...], b_s[kq * LANES : (kq + 1) * LANES, :], NT)
        for r in range(rows):
            at = (r * parts + kq) * chips
            flat[at : at + chips, :] = product[r * chips : (r + 1) * chips]
    exchange(s2, r2, 2, pack_rows(flat, s2))

    unpack(r2, spread, 2)

    def middle(r, kq):
        q = cols(kq, r)
        tri = jnp.concatenate(
            [spread[channels(g, r, kq), :] for g in range(tall)], axis=0
        )
        center = tri - jnp.mean(tri, axis=0, keepdims=True)
        scale = lax.rsqrt(jnp.mean(center * center, axis=0, keepdims=True) + EPS)
        hat = center * scale
        low = hat.astype(BF16)
        trilow_s[:, q] = low
        outputs = dot(outw_ref[...], low, TN)
        dl_s[:, q] = (outputs * e_s[:, q]).astype(BF16)
        d_hat = dh_s[:, q]
        m1 = jnp.mean(d_hat, axis=0, keepdims=True)
        m2 = jnp.mean(d_hat * hat, axis=0, keepdims=True)
        d_tri = scale * (d_hat - m1 - hat * m2)
        for g in range(tall):
            spread2[channels(g, r, kq), :] = d_tri[
                g * 8 : g * 8 + 8
            ]

    cells(middle, unroll=3)

    exchange(s3, r3, 3, pack(spread2, s3))

    share = 2 * side
    spot = col * 2 + core

    def put(w, value):
        n = w.shape[1]
        for m in range(share):
            w[m] = value[m * n : (m + 1) * n].astype(BF16)

    def line_peers(fn):
        for d in far:
            for e in range(2):
                if d or e:
                    fn((row * side + lax.rem(col + d, side)) * 2 + (1 - core if e else core))

    def send(src, dst, k, device):
        pltpu.make_async_remote_copy(
            src_ref=src,
            dst_ref=dst,
            send_sem=line_send.at[k],
            recv_sem=line_recv.at[k],
            device_id={"cells": device},
            device_id_type=MESH,
        ).start()

    def scatter_line(src, dst, k):
        line_peers(lambda p: send(src.at[lax.rem(p, share)], dst.at[spot], k, p))
        pltpu.make_async_copy(src.at[spot], dst.at[spot], line_recv.at[k]).start()

    def reduce_column(src, mid, dst, k):
        pltpu.make_async_copy(src, src, line_recv.at[k - 1]).wait()
        mid[...] = jnp.sum(src[...].astype(F32), axis=0)
        for d in far[:-1]:
            p = (lax.rem(row + d, side) * side + col) * 2 + core
            send(mid, dst.at[row], k, p)
        pltpu.make_async_copy(mid, dst.at[row], line_recv.at[k]).start()

    def gather_line(src, mid, dst, k):
        pltpu.make_async_copy(src, src, line_recv.at[k - 1]).wait()
        mid[...] = (jnp.sum(src[...], axis=0) * (1.0 / length)).astype(BF16)
        line_peers(lambda p: send(mid, dst.at[spot], k, p))
        pltpu.make_async_copy(mid, dst.at[spot], line_recv.at[k]).start()

    def drain(w, column, full, k):
        for e, (src, n) in enumerate(((full, share), (column, side), (full, share))):
            view = src.at[pl.ds(0, n - 1)]
            pltpu.make_async_copy(view, view, line_send.at[k + e]).wait()

    put(
        w1,
        jnp.concatenate(
            [
                dot(norm_s[...], dl_s[...], NT),
                dot(trilow_s[...], do_s[...], NT),
                jnp.zeros((width - hidden, width), F32),
            ],
            axis=0,
        ),
    )
    scatter_line(w1, line1, 0)

    def gate_part(r, kq):
        q = cols(kq, r)
        dn_s[:, q] = dot(gate_ref[...], dl_s[:, q], NN)

    cells(gate_part, unroll=3)

    unpack(r3, spread, 3)
    gather_rows(spread, dt_s, rows * parts)
    second = []
    for kq in range(parts):
        wide[kq] = dot(dt_s[...], a_s[:, kq * LANES : (kq + 1) * LANES], TN)
        for r in range(rows):
            for g in range(groups):
                half_s[kq, r * chips + g * 8 : r * chips + g * 8 + 8, :] = wide[
                    kq, pl.ds(g * 48 + 3 * (1 - core) + r, 8, stride=6), :
                ]
        second.append(to_partner(half_s.at[kq], half_r.at[kq], 1 + kq))
    for kq in range(parts):
        product = dot(dt_s[...], b_s[:, kq * LANES : (kq + 1) * LANES], NN)
        for r in range(rows):
            at = (r * parts + kq) * chips
            flat[at : at + chips, :] = product[r * chips : (r + 1) * chips]
    exchange(s4a, r4a, 4, pack_rows(flat, s4a), col_recv.at[0, col])
    for kq in range(parts):
        second[kq].wait()
        for r in range(rows):
            for g in range(groups):
                at = (r * parts + kq) * chips + g * 8
                flat[at : at + 8, :] = (
                    wide[kq, pl.ds(g * 48 + 3 * core + r, 8, stride=6), :]
                    + half_r[kq, r * chips + g * 8 : r * chips + g * 8 + 8, :]
                )
    exchange(s4b, r4b, 5, pack_rows(flat, s4b), col_recv.at[1, col])
    reduce_column(line1, mid1a, column1, 1)

    def half_back(ab, src, w, line, k):
        for d in reversed(far):
            x = lax.rem(col + d, side)
            view = src.at[pl.ds(0, side)]
            pltpu.make_async_copy(view, view, col_recv.at[ab, x]).wait()
            for y in range(side):
                for i in range(pairs):
                    few[y * SLOT + 2 * i : y * SLOT + 2 * i + 2, :] = src[
                        y * side + x, i
                    ].astype(F32)
            at = pl.ds(pl.multiple_of(ab * hidden + x * 8, 8), 8)
            to = pl.ds(pl.multiple_of(2 * (ab * hidden + x * 8), 16), 16)
            for r in range(rows):
                for kq in range(parts):
                    q = slice((r * parts + kq) * LANES, (r * parts + kq + 1) * LANES)
                    d_factors = few[pl.ds(r * parts + kq, 8, stride=SLOT), :]
                    both = [d_factors * p1_s[at, q], d_factors * p2_s[at, q]]
                    dproj_s[to, q] = jnp.concatenate(both, axis=0).astype(BF16)
            term = dot(dproj_s[to, :], norm_s[...], NT)
            across_line = (row * side + lax.rem(x + side // 2, side)) * 2
            for e in range(2):
                w[x, e] = term[8 * e : 8 * e + 8].astype(BF16)
            for e in range(2):
                half = 1 - core if e else core
                if e or d != side // 2:
                    send(w.at[x, half], line.at[spot], k, across_line + half)
                else:
                    pltpu.make_async_copy(w.at[x, half], line.at[spot], line_recv.at[k]).start()

    half_back(0, r4a, w2, line2, 3)
    half_back(1, r4b, w3, line3, 6)

    def finish(r, kq):
        q = cols(kq, r)
        d_norm = dot(projt_s[...], dproj_s[:, q], TN) + dn_s[:, q]
        zhat = zhat_s[:, q]
        m1 = jnp.mean(d_norm, axis=0, keepdims=True)
        m2 = jnp.mean(d_norm * zhat, axis=0, keepdims=True)
        grad = zscale_s[:, q] * (d_norm - m1 - zhat * m2)
        pair_out[q, :] = grad.T.astype(BF16)

    reduce_column(line2, mid2a, column2, 4)
    reduce_column(line3, mid3a, column3, 7)
    gather_line(column1, mid1b, full1, 2)
    cells(finish, unroll=3)
    gather_line(column2, mid2b, full2, 5)

    def landed(full, k):
        pltpu.make_async_copy(full, full, line_recv.at[k]).wait()
        return full[...].astype(F32).reshape(full.shape[0] * full.shape[1], width)

    gather_line(column3, mid3b, full3, 8)
    sums = landed(full1, 2)
    gate_out[...] = sums[0:width]
    out_out[...] = sums[width : width + hidden]
    for k, src in enumerate((s1b, s1a, s2, s3, s4a, s4b)):
        sent(src, k)
    pltpu.make_async_copy(r1p, r1p, pair_send.at[0]).wait()
    drain(w1, column1, full1, 0)
    drain(w2, column2, full2, 3)
    pltpu.make_async_copy(full2, full2, line_recv.at[5]).wait()
    pltpu.make_async_copy(full3, full3, line_recv.at[8]).wait()
    for e in range(2):
        turned = [
            full[2 * ((x + side // 2) % side) + e].astype(F32)
            for full in (full2, full3)
            for x in range(side)
        ]
        proj_out[:, e * width : (e + 1) * width] = jnp.concatenate(turned, axis=0).T
    drain(w3, column3, full3, 6)


def write(a_ref, b_ref, c_ref, d_ref, a_out, b_out, c_out, d_out, sem):
    copies = [
        pltpu.make_async_copy(src, dst, sem.at[k])
        for k, (src, dst) in enumerate(
            ((a_ref, a_out), (b_ref, b_out), (c_ref, c_out), (d_ref, d_out))
        )
    ]
    for copy in copies:
        copy.start()
    for copy in copies:
        copy.wait()


def local(
    pair_act, pair_mask, chain_ids, proj_weight, gate_weight, chain_bias, out_weight, out_grad
):
    devices = lax.axis_size("cells")
    chips = devices // 2
    rows, length, width = pair_act.shape
    hidden = out_weight.shape[0]
    count = rows * length
    parts = length // LANES
    side = math.isqrt(chips)
    assert side == 8 and hidden == chips
    share = 2 * side
    vm = pl.BlockSpec(memory_space=pltpu.VMEM)
    hbm = pl.BlockSpec(memory_space=pltpu.HBM)
    V = pltpu.VMEM
    pairs = (rows * parts + 1) // 2
    assert rows * parts == 2 * pairs - 1
    slots = (chips, pairs, 2, LANES)
    short = (chips, pairs - 1, 2, LANES)

    def reduction(block):
        return [
            V((share, block, width), BF16),
            V((share, block, width), BF16),
            V((block, width), F32),
            V((side, block, width), F32),
            V((block, width), BF16),
            V((share, block, width), BF16),
        ]

    def by_column(block):
        return [V((side, 2, block, width), BF16), *reduction(block)[1:]]

    shapes = (
        jax.ShapeDtypeStruct((count, width), BF16),
        jax.ShapeDtypeStruct((width, 4 * hidden), F32),
        jax.ShapeDtypeStruct((width, width), F32),
        jax.ShapeDtypeStruct((hidden, width), F32),
    )
    out = pl.pallas_call(
        kernel,
        out_shape=shapes,
        in_specs=8 * [hbm],
        out_specs=(vm, vm, vm, vm),
        scratch_shapes=[
            V((count, width), BF16),
            V((count, width), BF16),
            V((rows, length), jnp.int32),
            V((length,), jnp.int32),
            pltpu.SMEM((length,), jnp.int32),
            V((width, 4 * hidden), BF16),
            V((width, width), BF16),
            V((2, width), F32),
            V((hidden, width), BF16),
            pltpu.SemaphoreType.DMA((9,)),
            V((width, count), F32),
            V((1, count), F32),
            V((width, count), BF16),
            V((2 * hidden, count), F32),
            V((2 * hidden, count), F32),
            V((width, count), BF16),
            V((width, count), F32),
            V((hidden, count), F32),
            V((width, count), BF16),
            V((width, count), F32),
            V((hidden, count), BF16),
            V((4 * hidden, count), BF16),
            V((SLOT * chips + 8 * side, LANES), F32),
            V((parts, length, LANES), F32),
            V((2 * pairs * chips, LANES), F32),
            V((rows * chips, length), BF16),
            V((length, length), BF16),
            V((rows * chips, length), BF16),
            V((SLOT * chips + 8 * side, LANES), F32),
            V(short, BF16),
            *(5 * [V(slots, BF16)]),
            V(short, BF16),
            *(6 * [V(slots, BF16)]),
            V((parts, rows * chips, LANES), F32),
            V((parts, rows * chips, LANES), F32),
            *reduction(2 * width // share),
            V((8 * SLOT, LANES), F32),
            V((4 * hidden, width), BF16),
            pltpu.SemaphoreType.DMA((2, side)),
            *by_column(width // share),
            *by_column(width // share),
            pltpu.SemaphoreType.DMA((6,)),
            pltpu.SemaphoreType.DMA((4, side)),
            pltpu.SemaphoreType.DMA((1 + parts,)),
            pltpu.SemaphoreType.DMA((1 + parts,)),
            pltpu.SemaphoreType.DMA((9,)),
            pltpu.SemaphoreType.DMA((9,)),
        ],
        compiler_params=pltpu.CompilerParams(
            collective_id=0, has_side_effects=True, vmem_limit_bytes=20 * 1024 * 1024
        ),
    )(
        *(
            pltpu.with_memory_space_constraint(x, pltpu.HBM)
            for x in (
                pair_act.reshape(count, width),
                out_grad.reshape(count, width),
                pair_mask,
                chain_ids,
                proj_weight,
                gate_weight,
                chain_bias,
                out_weight,
            )
        )
    )
    out = pl.pallas_call(
        write,
        out_shape=shapes,
        in_specs=4 * [vm],
        out_specs=tuple(4 * [hbm]),
        scratch_shapes=[pltpu.SemaphoreType.DMA((4,))],
        compiler_params=pltpu.CompilerParams(vmem_limit_bytes=4 * 1024 * 1024),
    )(*out)
    return (out[0].reshape(rows, length, width), out[1], out[2], out[3])


def solution(mesh):
    placed = (
        P(("groups", "cells"), None, None),
        P(("groups", "cells"), None),
        P("groups"),
        P(),
        P(),
        P(),
        P(),
        P(("groups", "cells"), None, None),
    )
    return jax.shard_map(
        local,
        mesh=mesh,
        in_specs=placed,
        out_specs=(
            P(("groups", "cells"), None, None),
            P("groups", None),
            P("groups", None),
            P("groups", None),
        ),
        check_vma=False,
    )
```

```python
import math

import jax
import jax.numpy as jnp
from jax import lax
from jax.experimental import pallas as pl
from jax.experimental.pallas import tpu as pltpu
from jax.sharding import PartitionSpec as P

EPS = 1e-05
MESH = pl.DeviceIdType.MESH
F32 = jnp.float32
BF16 = jnp.bfloat16
LANES = 128
SLOT = 24
NT = (((1,), (1,)), ((), ()))
TN = (((0,), (0,)), ((), ()))
NN = (((1,), (0,)), ((), ()))


def dot(a, b, dims):
    return lax.dot_general(a, b, dims, preferred_element_type=F32)


def loop(n, body, unroll=1):
    def step(i, carry):
        body(i)
        return carry

    lax.fori_loop(0, n, step, 0, unroll=unroll)


def kernel(
    act_hbm,
    grad_hbm,
    mask_hbm,
    chain_hbm,
    proj_hbm,
    gate_hbm,
    bias_hbm,
    outw_hbm,
    pair_out,
    proj_out,
    gate_out,
    out_out,
    act_ref,
    grad_ref,
    mask_ref,
    chain_ref,
    own_ref,
    proj_ref,
    gate_ref,
    bias_ref,
    outw_ref,
    in_sem,
    zhat_s,
    zscale_s,
    norm_s,
    p1_s,
    p2_s,
    do_s,
    e_s,
    dh_s,
    dl_s,
    dn_s,
    trilow_s,
    dproj_s,
    spread,
    wide,
    flat,
    a_s,
    b_s,
    dt_s,
    spread2,
    s1a,
    s1b,
    s2,
    s3,
    s4a,
    s4b,
    r1a,
    r1b,
    r1p,
    r2,
    r3,
    r4a,
    r4b,
    half_s,
    half_r,
    w1,
    line1,
    mid1a,
    column1,
    mid1b,
    full1,
    few,
    projt_s,
    col_recv,
    w2,
    line2,
    mid2a,
    column2,
    mid2b,
    full2,
    w3,
    line3,
    mid3a,
    column3,
    mid3b,
    full3,
    send_sem,
    recv_sem,
    pair_send,
    pair_recv,
    line_send,
    line_recv,
):
    loads = [
        pltpu.make_async_copy(src, dst, in_sem.at[k])
        for k, (src, dst) in enumerate(
            (
                (act_hbm, act_ref),
                (proj_hbm, proj_ref),
                (mask_hbm, mask_ref),
                (grad_hbm, grad_ref),
                (gate_hbm, gate_ref),
                (outw_hbm, outw_ref),
                (bias_hbm, bias_ref),
                (chain_hbm, chain_ref),
                (chain_hbm, own_ref),
            )
        )
    ]
    for load in loads:
        load.start()
    me = lax.axis_index("cells")
    devices = lax.axis_size("cells")
    chips = devices // 2
    side = math.isqrt(chips)
    chip = me // 2
    core = lax.rem(me, 2)
    row, col = chip // side, lax.rem(chip, side)
    far = sorted(range(side), key=lambda d: -min(d, side - d))
    partner = me + 1 - 2 * core
    rows, length = mask_ref.shape
    width = act_ref.shape[1]
    hidden = outw_ref.shape[0]
    parts = length // LANES
    tall = hidden // 8
    groups = chips // 8
    pairs = (rows * parts + 1) // 2

    barrier = pltpu.get_barrier_semaphore()

    def line_of(i):
        step = side // 2 + ((i + 1) // 2) * (1 - 2 * lax.rem(i, 2))
        return lax.rem(row + step, side)

    def each_chip(fn, prepare=None):
        def line(i):
            now, later = line_of(i), line_of(i + 1)
            for x, d in enumerate(far):
                if prepare is not None:
                    prepare(later, x)
                fn(now * side + lax.rem(col + d, side))

        if prepare is not None:
            for x in range(side):
                prepare(line_of(jnp.int32(0)), x)
        loop(side - 1, line)
        for d in far[:-1]:
            fn(row * side + lax.rem(col + d, side))

    def greet(peer):
        pl.semaphore_signal(barrier, inc=1, device_id={"cells": peer}, device_id_type=MESH)

    each_chip(lambda t: greet(t * 2 + core))
    for d in far[:-1]:
        greet((row * side + lax.rem(col + d, side)) * 2 + 1 - core)
    greet(partner)

    def exchange(src, dst, k, prepare=None, recv=None):
        recv = recv_sem.at[k, row] if recv is None else recv

        def one(t):
            pltpu.make_async_remote_copy(
                src_ref=src.at[t],
                dst_ref=dst.at[chip],
                send_sem=send_sem.at[k],
                recv_sem=recv,
                device_id={"cells": t * 2 + core},
                device_id_type=MESH,
            ).start()

        each_chip(one, prepare)
        pltpu.make_async_copy(src.at[chip], dst.at[chip], recv).start()

    def sent(src, k):
        view = src.at[pl.ds(0, chips - 1)]
        pltpu.make_async_copy(view, view, send_sem.at[k]).wait()

    def to_partner(src, dst, k):
        copy = pltpu.make_async_remote_copy(
            src_ref=src,
            dst_ref=dst,
            send_sem=pair_send.at[k],
            recv_sem=pair_recv.at[k],
            device_id={"cells": partner},
            device_id_type=MESH,
        )
        copy.start()
        return copy

    def cols(kq, r=0):
        return pl.ds(pl.multiple_of((r * parts + kq) * LANES, LANES), LANES)

    def cells(body, unroll=1):
        for r in range(rows):
            loop(parts, lambda kq, r=r: body(r, kq), unroll)

    lead = side * SLOT + 8

    def slot(y, x):
        return pl.multiple_of(y * lead + x * SLOT, 8)

    def unpack(src, dst, k=None, then=None):
        def one(i):
            y = line_of(side - 1 - i)
            line = pl.ds(y * side, side)
            if k is not None:
                pltpu.make_async_copy(src.at[line], src.at[line], recv_sem.at[k, y]).wait()
            if then is not None:
                then(line)
            for x in range(side):
                for i in range(src.shape[1]):
                    dst[pl.ds(slot(y, x) + 2 * i, 2), :] = src[y * side + x, i].astype(F32)

        loop(side, one)

    def pack(src, dst):
        def one(y, x):
            for i in range(dst.shape[1]):
                at = pl.ds(slot(y, x) + 2 * i, 2)
                dst[y * side + x, i] = src[at, :].astype(BF16)

        return one

    def pack_rows(src, dst):
        def one(y, x):
            t = y * side + x
            for i in range(pairs):
                dst[t, i] = src[pl.ds(2 * i * chips + t, 2, stride=chips), :].astype(BF16)

        return one

    def eight(src, g, r, kq):
        return src[pl.ds(g * lead + r * parts + kq, 8, stride=SLOT), :]

    def channels(g, r, kq):
        return pl.ds(g * SLOT + r * parts + kq, 8, stride=lead)

    def gather_row(src, dst, r, kq, start):
        for g in range(0, groups, 2):
            at = r * chips + g * 8
            dst[at : at + 16, kq * LANES : (kq + 1) * LANES] = jnp.concatenate(
                [eight(src, g, 0, start), eight(src, g + 1, 0, start)], axis=0
            ).astype(BF16)

    def gather_rows(src, dst, n):
        for k in range(n):
            gather_row(src, dst, k // parts, k % parts, k)

    eye = (
        lax.broadcasted_iota(jnp.int32, (width, width), 0)
        == lax.broadcasted_iota(jnp.int32, (width, width), 1)
    ).astype(BF16)

    for load in loads[:3]:
        load.wait()

    def front(r, kq):
        q = cols(kq, r)
        z = dot(eye, act_ref[q, :], NT)
        center = z - jnp.mean(z, axis=0, keepdims=True)
        scale = lax.rsqrt(jnp.mean(center * center, axis=0, keepdims=True) + EPS)
        zhat = center * scale
        low = zhat.astype(BF16)
        zhat_s[:, q] = zhat
        zscale_s[:, q] = scale
        norm_s[:, q] = low
        projected = dot(proj_ref[...], low, TN)
        keeper = mask_ref[r : r + 1, cols(kq)].astype(F32)
        values = projected[: 2 * hidden]
        sigma = jax.nn.sigmoid(projected[2 * hidden :])
        p1 = keeper * sigma
        factors = p1 * values
        p1_s[:, q] = p1
        p2_s[:, q] = factors * (1.0 - sigma)
        for ab in range(2):
            for g in range(tall):
                at = ab * hidden + g * 8
                (spread, spread2)[ab][
                    channels(g, r, kq), :
                ] = factors[at : at + 8]
                if ab == 0 and r == rows - 1:
                    spread2[channels(g, rows, 0), :] = factors[at : at + 8]

    cells(front, unroll=3)
    def pack_all(y):
        for src, dst in ((spread2, s1b), (spread, s1a)):
            for x in range(side):
                pack(src, dst)(y, x)

    loop(side, pack_all)
    pl.semaphore_wait(barrier, chips + side - 1)
    exchange(s1b, r1b, 0)
    exchange(s1a, r1a, 1)

    for load in loads[3:]:
        load.wait()
    within, across = (
        jnp.sum(eye.astype(F32) * bias_ref[e : e + 1, :], axis=1, keepdims=True) for e in range(2)
    )
    def gating(r, kq):
        q = cols(kq, r)
        same = chain_ref[cols(kq)].reshape(1, LANES) == own_ref[me * rows + r]
        logits = dot(gate_ref[...], norm_s[:, q], TN)
        logits = logits + jnp.where(same, within, across)
        gate = jax.nn.sigmoid(logits)
        up = dot(eye, grad_ref[q, :], NT) * gate
        low = up.astype(BF16)
        do_s[:, q] = low
        e_s[:, q] = up * (1.0 - gate)
        dh_s[:, q] = dot(outw_ref[...], low, NN)

    cells(gating, unroll=3)
    flipped = proj_ref[...].astype(F32).T
    for ab in range(2):
        for x in range(side):
            both = [
                flipped[(2 * e + ab) * hidden + x * 8 : (2 * e + ab) * hidden + x * 8 + 8]
                for e in range(2)
            ]
            at = 2 * (ab * hidden + x * 8)
            projt_s[at : at + 16, :] = jnp.concatenate(both, axis=0).astype(BF16)

    unpack(r1b, spread2, 0, lambda at: to_partner(r1b.at[at], r1p.at[at], 0))

    def place_right(src, which):
        for r in range(rows):
            for g in range(groups):
                for kq in range(parts):
                    wide[kq, pl.ds(g * 48 + 3 * which + r, 8, stride=6), :] = eight(src, g, r, kq)

    place_right(spread2, core)
    gather_row(spread2, a_s, rows - 1, parts - 1, rows * parts)
    pltpu.make_async_copy(r1p, r1p, pair_recv.at[0]).wait()
    unpack(r1p, spread2)
    place_right(spread2, 1 - core)
    unpack(r1a, spread, 1)
    gather_rows(spread, a_s, rows * parts - 1)
    for kq in range(parts):
        b_s[:, kq * LANES : (kq + 1) * LANES] = wide[kq].astype(BF16)
    for kq in range(parts):
        product = dot(a_s[...], b_s[kq * LANES : (kq + 1) * LANES, :], NT)
        for r in range(rows):
            at = (r * parts + kq) * chips
            flat[at : at + chips, :] = product[r * chips : (r + 1) * chips]
    exchange(s2, r2, 2, pack_rows(flat, s2))

    unpack(r2, spread, 2)

    def middle(r, kq):
        q = cols(kq, r)
        tri = jnp.concatenate(
            [spread[channels(g, r, kq), :] for g in range(tall)], axis=0
        )
        center = tri - jnp.mean(tri, axis=0, keepdims=True)
        scale = lax.rsqrt(jnp.mean(center * center, axis=0, keepdims=True) + EPS)
        hat = center * scale
        low = hat.astype(BF16)
        trilow_s[:, q] = low
        outputs = dot(outw_ref[...], low, TN)
        dl_s[:, q] = (outputs * e_s[:, q]).astype(BF16)
        d_hat = dh_s[:, q]
        m1 = jnp.mean(d_hat, axis=0, keepdims=True)
        m2 = jnp.mean(d_hat * hat, axis=0, keepdims=True)
        d_tri = scale * (d_hat - m1 - hat * m2)
        for g in range(tall):
            spread2[channels(g, r, kq), :] = d_tri[
                g * 8 : g * 8 + 8
            ]

    cells(middle, unroll=3)

    exchange(s3, r3, 3, pack(spread2, s3))

    share = 2 * side
    spot = col * 2 + core

    def put(w, value):
        n = w.shape[1]
        for m in range(share):
            w[m] = value[m * n : (m + 1) * n].astype(BF16)

    def line_peers(fn):
        for d in far:
            for e in range(2):
                if d or e:
                    fn((row * side + lax.rem(col + d, side)) * 2 + (1 - core if e else core))

    def send(src, dst, k, device):
        pltpu.make_async_remote_copy(
            src_ref=src,
            dst_ref=dst,
            send_sem=line_send.at[k],
            recv_sem=line_recv.at[k],
            device_id={"cells": device},
            device_id_type=MESH,
        ).start()

    def scatter_line(src, dst, k):
        line_peers(lambda p: send(src.at[lax.rem(p, share)], dst.at[spot], k, p))
        pltpu.make_async_copy(src.at[spot], dst.at[spot], line_recv.at[k]).start()

    def reduce_column(src, mid, dst, k):
        pltpu.make_async_copy(src, src, line_recv.at[k - 1]).wait()
        mid[...] = jnp.sum(src[...].astype(F32), axis=0)
        for d in far[:-1]:
            p = (lax.rem(row + d, side) * side + col) * 2 + core
            send(mid, dst.at[row], k, p)
        pltpu.make_async_copy(mid, dst.at[row], line_recv.at[k]).start()

    def gather_line(src, mid, dst, k):
        pltpu.make_async_copy(src, src, line_recv.at[k - 1]).wait()
        mid[...] = (jnp.sum(src[...], axis=0) * (1.0 / length)).astype(BF16)
        line_peers(lambda p: send(mid, dst.at[spot], k, p))
        pltpu.make_async_copy(mid, dst.at[spot], line_recv.at[k]).start()

    def drain(w, column, full, k):
        for e, (src, n) in enumerate(((full, share), (column, side), (full, share))):
            view = src.at[pl.ds(0, n - 1)]
            pltpu.make_async_copy(view, view, line_send.at[k + e]).wait()

    put(
        w1,
        jnp.concatenate(
            [
                dot(norm_s[...], dl_s[...], NT),
                dot(trilow_s[...], do_s[...], NT),
                jnp.zeros((width - hidden, width), F32),
            ],
            axis=0,
        ),
    )
    scatter_line(w1, line1, 0)

    def gate_part(r, kq):
        q = cols(kq, r)
        dn_s[:, q] = dot(gate_ref[...], dl_s[:, q], NN)

    cells(gate_part, unroll=3)

    unpack(r3, spread, 3)
    gather_rows(spread, dt_s, rows * parts)
    second = []
    for kq in range(parts):
        wide[kq] = dot(dt_s[...], a_s[:, kq * LANES : (kq + 1) * LANES], TN)
        for r in range(rows):
            for g in range(groups):
                half_s[kq, r * chips + g * 8 : r * chips + g * 8 + 8, :] = wide[
                    kq, pl.ds(g * 48 + 3 * (1 - core) + r, 8, stride=6), :
                ]
        second.append(to_partner(half_s.at[kq], half_r.at[kq], 1 + kq))
    for kq in range(parts):
        product = dot(dt_s[...], b_s[:, kq * LANES : (kq + 1) * LANES], NN)
        for r in range(rows):
            at = (r * parts + kq) * chips
            flat[at : at + chips, :] = product[r * chips : (r + 1) * chips]
    exchange(s4a, r4a, 4, pack_rows(flat, s4a), col_recv.at[0, col])
    for kq in range(parts):
        second[kq].wait()
        for r in range(rows):
            for g in range(groups):
                at = (r * parts + kq) * chips + g * 8
                flat[at : at + 8, :] = (
                    wide[kq, pl.ds(g * 48 + 3 * core + r, 8, stride=6), :]
                    + half_r[kq, r * chips + g * 8 : r * chips + g * 8 + 8, :]
                )
    exchange(s4b, r4b, 5, pack_rows(flat, s4b), col_recv.at[1, col])
    reduce_column(line1, mid1a, column1, 1)

    def half_back(ab, src, w, line, k, ahead=None):
        for d in reversed(far):
            if ahead is not None and d == side // 2:
                ahead()
            x = lax.rem(col + d, side)
            view = src.at[pl.ds(0, side)]
            pltpu.make_async_copy(view, view, col_recv.at[ab, x]).wait()
            for y in range(side):
                for i in range(pairs):
                    few[y * SLOT + 2 * i : y * SLOT + 2 * i + 2, :] = src[
                        y * side + x, i
                    ].astype(F32)
            at = pl.ds(pl.multiple_of(ab * hidden + x * 8, 8), 8)
            to = pl.ds(pl.multiple_of(2 * (ab * hidden + x * 8), 16), 16)
            for r in range(rows):
                for kq in range(parts):
                    q = slice((r * parts + kq) * LANES, (r * parts + kq + 1) * LANES)
                    d_factors = few[pl.ds(r * parts + kq, 8, stride=SLOT), :]
                    both = [d_factors * p1_s[at, q], d_factors * p2_s[at, q]]
                    dproj_s[to, q] = jnp.concatenate(both, axis=0).astype(BF16)
            term = dot(dproj_s[to, :], norm_s[...], NT)
            across_line = (row * side + lax.rem(x + side // 2, side)) * 2
            for e in range(2):
                w[x, e] = term[8 * e : 8 * e + 8].astype(BF16)
            for e in range(2):
                half = 1 - core if e else core
                if e or d != side // 2:
                    send(w.at[x, half], line.at[spot], k, across_line + half)
                else:
                    pltpu.make_async_copy(w.at[x, half], line.at[spot], line_recv.at[k]).start()

    half_back(0, r4a, w2, line2, 3)
    half_back(1, r4b, w3, line3, 6, lambda: reduce_column(line2, mid2a, column2, 4))

    def finish(r, kq):
        q = cols(kq, r)
        d_norm = dot(projt_s[...], dproj_s[:, q], TN) + dn_s[:, q]
        zhat = zhat_s[:, q]
        m1 = jnp.mean(d_norm, axis=0, keepdims=True)
        m2 = jnp.mean(d_norm * zhat, axis=0, keepdims=True)
        grad = zscale_s[:, q] * (d_norm - m1 - zhat * m2)
        pair_out[q, :] = grad.T.astype(BF16)

    reduce_column(line3, mid3a, column3, 7)
    gather_line(column1, mid1b, full1, 2)
    cells(finish, unroll=3)
    gather_line(column2, mid2b, full2, 5)

    def landed(full, k):
        pltpu.make_async_copy(full, full, line_recv.at[k]).wait()
        return full[...].astype(F32).reshape(full.shape[0] * full.shape[1], width)

    gather_line(column3, mid3b, full3, 8)
    sums = landed(full1, 2)
    gate_out[...] = sums[0:width]
    out_out[...] = sums[width : width + hidden]
    for k, src in enumerate((s1b, s1a, s2, s3, s4a, s4b)):
        sent(src, k)
    pltpu.make_async_copy(r1p, r1p, pair_send.at[0]).wait()
    drain(w1, column1, full1, 0)
    drain(w2, column2, full2, 3)
    pltpu.make_async_copy(full2, full2, line_recv.at[5]).wait()
    pltpu.make_async_copy(full3, full3, line_recv.at[8]).wait()
    for e in range(2):
        turned = [
            full[2 * ((x + side // 2) % side) + e].astype(F32)
            for full in (full2, full3)
            for x in range(side)
        ]
        proj_out[:, e * width : (e + 1) * width] = jnp.concatenate(turned, axis=0).T
    drain(w3, column3, full3, 6)


def write(a_ref, b_ref, c_ref, d_ref, a_out, b_out, c_out, d_out, sem):
    copies = [
        pltpu.make_async_copy(src, dst, sem.at[k])
        for k, (src, dst) in enumerate(
            ((a_ref, a_out), (b_ref, b_out), (c_ref, c_out), (d_ref, d_out))
        )
    ]
    for copy in copies:
        copy.start()
    for copy in copies:
        copy.wait()


def local(
    pair_act, pair_mask, chain_ids, proj_weight, gate_weight, chain_bias, out_weight, out_grad
):
    devices = lax.axis_size("cells")
    chips = devices // 2
    rows, length, width = pair_act.shape
    hidden = out_weight.shape[0]
    count = rows * length
    parts = length // LANES
    side = math.isqrt(chips)
    assert side == 8 and hidden == chips
    share = 2 * side
    vm = pl.BlockSpec(memory_space=pltpu.VMEM)
    hbm = pl.BlockSpec(memory_space=pltpu.HBM)
    V = pltpu.VMEM
    pairs = (rows * parts + 1) // 2
    assert rows * parts == 2 * pairs - 1
    slots = (chips, pairs, 2, LANES)
    short = (chips, pairs - 1, 2, LANES)

    def reduction(block):
        return [
            V((share, block, width), BF16),
            V((share, block, width), BF16),
            V((block, width), F32),
            V((side, block, width), F32),
            V((block, width), BF16),
            V((share, block, width), BF16),
        ]

    def by_column(block):
        return [V((side, 2, block, width), BF16), *reduction(block)[1:]]

    shapes = (
        jax.ShapeDtypeStruct((count, width), BF16),
        jax.ShapeDtypeStruct((width, 4 * hidden), F32),
        jax.ShapeDtypeStruct((width, width), F32),
        jax.ShapeDtypeStruct((hidden, width), F32),
    )
    out = pl.pallas_call(
        kernel,
        out_shape=shapes,
        in_specs=8 * [hbm],
        out_specs=(vm, vm, vm, vm),
        scratch_shapes=[
            V((count, width), BF16),
            V((count, width), BF16),
            V((rows, length), jnp.int32),
            V((length,), jnp.int32),
            pltpu.SMEM((length,), jnp.int32),
            V((width, 4 * hidden), BF16),
            V((width, width), BF16),
            V((2, width), F32),
            V((hidden, width), BF16),
            pltpu.SemaphoreType.DMA((9,)),
            V((width, count), F32),
            V((1, count), F32),
            V((width, count), BF16),
            V((2 * hidden, count), F32),
            V((2 * hidden, count), F32),
            V((width, count), BF16),
            V((width, count), F32),
            V((hidden, count), F32),
            V((width, count), BF16),
            V((width, count), F32),
            V((hidden, count), BF16),
            V((4 * hidden, count), BF16),
            V((SLOT * chips + 8 * side, LANES), F32),
            V((parts, length, LANES), F32),
            V((2 * pairs * chips, LANES), F32),
            V((rows * chips, length), BF16),
            V((length, length), BF16),
            V((rows * chips, length), BF16),
            V((SLOT * chips + 8 * side, LANES), F32),
            V(short, BF16),
            *(5 * [V(slots, BF16)]),
            V(short, BF16),
            *(6 * [V(slots, BF16)]),
            V((parts, rows * chips, LANES), F32),
            V((parts, rows * chips, LANES), F32),
            *reduction(2 * width // share),
            V((8 * SLOT, LANES), F32),
            V((4 * hidden, width), BF16),
            pltpu.SemaphoreType.DMA((2, side)),
            *by_column(width // share),
            *by_column(width // share),
            pltpu.SemaphoreType.DMA((6,)),
            pltpu.SemaphoreType.DMA((4, side)),
            pltpu.SemaphoreType.DMA((1 + parts,)),
            pltpu.SemaphoreType.DMA((1 + parts,)),
            pltpu.SemaphoreType.DMA((9,)),
            pltpu.SemaphoreType.DMA((9,)),
        ],
        compiler_params=pltpu.CompilerParams(
            collective_id=0, has_side_effects=True, vmem_limit_bytes=20 * 1024 * 1024
        ),
    )(
        *(
            pltpu.with_memory_space_constraint(x, pltpu.HBM)
            for x in (
                pair_act.reshape(count, width),
                out_grad.reshape(count, width),
                pair_mask,
                chain_ids,
                proj_weight,
                gate_weight,
                chain_bias,
                out_weight,
            )
        )
    )
    out = pl.pallas_call(
        write,
        out_shape=shapes,
        in_specs=4 * [vm],
        out_specs=tuple(4 * [hbm]),
        scratch_shapes=[pltpu.SemaphoreType.DMA((4,))],
        compiler_params=pltpu.CompilerParams(vmem_limit_bytes=4 * 1024 * 1024),
    )(*out)
    return (out[0].reshape(rows, length, width), out[1], out[2], out[3])


def solution(mesh):
    placed = (
        P(("groups", "cells"), None, None),
        P(("groups", "cells"), None),
        P("groups"),
        P(),
        P(),
        P(),
        P(),
        P(("groups", "cells"), None, None),
    )
    return jax.shard_map(
        local,
        mesh=mesh,
        in_specs=placed,
        out_specs=(
            P(("groups", "cells"), None, None),
            P("groups", None),
            P("groups", None),
            P("groups", None),
        ),
        check_vma=False,
    )
```
